256 devices in a mesh: section: 2 (over y_lo), expert: 8 (over y_hi, x), tensor: 16 (over z, core).
Axes of the slice: x: 4, y: 4 (y_hi: 2, y_lo: 2; y = y_hi * 2 + y_lo), z: 8, core: 2. Of those that a mesh axis runs over, the one named last changes fastest.
Arguments:
- query: bfloat16 [8, 1024, 4096], P('expert', 'tensor', 'section'), may hold values from -24 to 24
- keys: bfloat16 [8, 1024, 1024], P('expert', 'tensor', 'section'), may hold values from -24 to 24
- values: bfloat16 [8, 1024, 1024], P('expert', 'tensor', 'section'), may hold values from -6 to 6
- residual: bfloat16 [8, 1024, 4096], P('expert', 'tensor', 'section'), may hold values from -6 to 6
- routes: int32 [8, 1024, 2], P('expert', 'tensor'), may hold values from 0 to 7, all different within a row; in each aligned block of 64 rows (0 to 63, 64 to 127, ..., all dimensions but the last counted through in order) at most 17 rows name the same one
- gates: float32 [8, 1024, 2], P('expert', 'tensor'), may hold values from 0.1 to 0.9
- w_gate: bfloat16 [8, 4096, 8192], P('expert', None, 'tensor'), may hold values from -0.09375 to 0.09375
- w_up: bfloat16 [8, 4096, 8192], P('expert', None, 'tensor'), may hold values from -0.09375 to 0.09375
- w_down: bfloat16 [8, 8192, 4096], P('expert', 'tensor'), may hold values from -0.0625 to 0.0625
Outputs:
- layer_out: bfloat16 [8, 1024, 4096], P('expert', 'tensor', 'section')
The draws below stay inside these ranges and needn't reach their ends.
Inputs may be any that keep to these rules, and one draw needn't show every extreme that they name: `routes`: the 2 entries of a row differ. In the rows of one index of expert and tensor (aligned blocks of 64 positions, taken in order over sequences and positions) no expert is named more than 17 times.
All inputs are finite; a program needn't handle non-finite values.
Results may differ from the reference program's by a relative error of at most 0.014.
Values may be sent and summed in bfloat16 or wider, within the bound.
A program may use at most 128 MiB of HBM per device.

```python
import math
import jax
import jax.numpy as jnp
import numpy as np
from jax import lax

D = 4096
H = 32
KVH = 8
HD = 128
EXPERTS = 8
TOP = 2
FF = 8192
TOK_DEV = 64
CAP = 17
GROUPS = 16
SEQS = 8
LENGTH = 1024
N_EXPERT = 8
N_TENSOR = 16


def attention_pair(key):
    key_noise = jnp.clip(jax.random.normal(jax.random.fold_in(key, 11), (SEQS, LENGTH, KVH * HD), jnp.float32), -4.5, 4.5)
    query_noise = jnp.clip(jax.random.normal(jax.random.fold_in(key, 12), (SEQS, LENGTH, H * HD), jnp.float32), -4.5, 4.5)
    key_field = key_noise
    query_field = query_noise
    return (query_field, key_field)


def draw_query(key, part):
    return attention_pair(key)[0].astype(jnp.bfloat16)


def draw_keys(key, part):
    return attention_pair(key)[1].astype(jnp.bfloat16)


def block_scale(stream_key, shape, pieces, low, high):
    level, own = 1.0, jax.random.fold_in(stream_key, 6)
    for axis_at, parts in pieces:
        heights = jnp.exp(jax.random.uniform(jax.random.fold_in(own, axis_at), (parts,), jnp.float32, low / len(pieces), high / len(pieces)))
        level = level * jnp.repeat(heights, shape[axis_at] // parts).reshape([-1 if axis == axis_at else 1 for axis in range(len(shape))])
    return level


def deal_out(rng, own, number, rows, amount, top, reach, slope):
    ranking = jax.random.permutation(rng, amount)
    crowded, common = portions_of(amount, rows * top, reach, slope, True), portions_of(amount, rows * top, reach, slope, False)
    places = jnp.arange(amount)

    def named(tallies, rotation):
        used = int((tallies > 0).sum())
        fixed = max(1, used // 4)
        moved = fixed + (places - fixed + rotation * (used - fixed)) % max(1, amount - fixed)
        return jnp.zeros((amount,), jnp.int32).at[ranking[jnp.where(places < fixed, places, moved)]].set(jnp.asarray(tallies, jnp.int32))

    tallies = jnp.where(number % 4 == 0, named(crowded, number // 4), named(common, number - number // 4 - 1))
    mixed = jax.random.permutation(jax.random.fold_in(own, 3), amount)
    donor, sink = mixed[0:amount // 2 * 2:2], mixed[1:amount // 2 * 2:2]
    slack = jnp.minimum(tallies[donor] - 1, reach - tallies[sink]) // 2
    slack = jnp.where((donor == ranking[0]) | (sink == ranking[0]) | (tallies[sink] == 0), 0, jnp.maximum(slack, 0))
    moved = jax.random.randint(jax.random.fold_in(own, 4), (amount // 2,), 0, 1 << 20) % (slack + 1)
    tallies = tallies.at[donor].add(-moved).at[sink].add(moved)
    labels = jnp.searchsorted(jnp.cumsum(tallies), jnp.arange(rows * top), side="right").astype(jnp.int32)
    listing = labels.reshape(top, rows).T
    listing = listing[jax.random.permutation(jax.random.fold_in(own, 1), rows)]
    rotation = jax.random.randint(jax.random.fold_in(own, 2), (rows, 1), 0, top)
    return jnp.take_along_axis(listing, (jnp.arange(top)[None, :] + rotation) % top, axis=1)


def portions_of(number_of, total, most, skew, full):
    loads = [(1 << 20) // math.isqrt(standing ** skew) + 1 for standing in range(1, number_of + 1)]
    largest = most if full else min(most, max(-(-total // number_of), total * loads[0] // sum(loads)))
    least = 1 if total - largest >= number_of - 1 else 0
    counts, surplus = [largest] + [least] * (number_of - 1), total - largest - least * (number_of - 1)
    while surplus > 0:
        candidates = [i for i in range(1, number_of) if counts[i] < largest] or [i for i in range(1, number_of) if counts[i] < most]
        pool, remaining = sum([loads[i] for i in candidates]), surplus
        for i in candidates:
            more = min(most - counts[i], max(1, remaining * loads[i] // pool), surplus)
            counts[i] = counts[i] + more
            surplus = surplus - more
    return np.array(counts)


def gaussian(own_key, dims, scale, bound, shards=(), held_as=jnp.bfloat16):
    factor_of = block_scale(own_key, dims, shards, -0.22, 0.18) if shards else 1.0
    array = jax.random.normal(own_key, dims, jnp.float32) * scale * factor_of
    return jnp.minimum(jnp.maximum(array, -bound), bound).astype(held_as)


def setup_inputs(seed: int = 0) -> dict:
    seeds = jax.random.split(jax.random.key(seed), 10)
    query = draw_query(jax.random.fold_in(seeds[9], 71), 0)
    keys = draw_keys(jax.random.fold_in(seeds[9], 71), 0)
    values = gaussian(seeds[2], (SEQS, LENGTH, KVH * HD), 1.0, 6.0, ((0, 8), (1, 16), (2, 2)))
    residual = gaussian(seeds[3], (SEQS, LENGTH, D), 1.0, 6.0, ((0, 8), (1, 16), (2, 2)))
    routes_keys = jax.random.split(jax.random.fold_in(seeds[4], 1), SEQS * LENGTH // TOK_DEV)
    routes_turns = jax.random.permutation(jax.random.fold_in(seeds[4], 3), SEQS * LENGTH // TOK_DEV)
    routes = jax.vmap(lambda own, number: deal_out(jax.random.fold_in(seeds[4], 2), own, number, TOK_DEV, EXPERTS, TOP, CAP, 2))(routes_keys, routes_turns).reshape((SEQS, LENGTH, TOP))
    gates = jnp.clip(0.1 + 0.79999997 * jax.random.uniform(seeds[5], (SEQS, LENGTH, TOP), jnp.float32) ** block_scale(seeds[5], (SEQS, LENGTH, TOP), ((0, 8), (1, 16)), -0.2, 0.2), 0.1, 0.9)
    w_gate = gaussian(seeds[6], (EXPERTS, D, FF), D ** -0.5, 0.09375, ((0, 8), (2, 16)))
    w_up = gaussian(seeds[7], (EXPERTS, D, FF), D ** -0.5, 0.09375, ((0, 8), (2, 16)))
    w_down = gaussian(seeds[8], (EXPERTS, FF, D), FF ** -0.5, 0.0625, ((0, 8), (1, 16)))
    return dict(query=query, keys=keys, values=values, residual=residual, routes=routes, gates=gates, w_gate=w_gate, w_up=w_up, w_down=w_down)


def attend(query_seq, key_seq, value_seq):
    length = query_seq.shape[0]
    groups = H // KVH
    queries = query_seq.reshape(length, KVH, groups, HD).astype(jnp.float32)
    keys_all = key_seq.reshape(length, KVH, HD).astype(jnp.float32)
    values_all = value_seq.reshape(length, KVH, HD).astype(jnp.float32)
    scores = jnp.einsum('qkgd,tkd->kgqt', queries, keys_all) / math.sqrt(HD)
    positions = jnp.arange(length)
    causal = positions[:, None] >= positions[None, :]
    masked = jnp.where(causal, scores, -1e+30)
    row_peak = lax.optimization_barrier(jnp.max(masked, axis=-1, keepdims=True))
    exp_terms = jnp.where(causal, jnp.exp(masked - row_peak), 0.0)
    weights = (exp_terms / lax.optimization_barrier(jnp.sum(exp_terms, axis=-1, keepdims=True))).astype(jnp.bfloat16)
    context = jnp.einsum('kgqt,tkd->qkgd', weights.astype(jnp.float32), values_all)
    return context.reshape(length, H * HD)

def reference(query, keys, values, residual, routes, gates, w_gate, w_up, w_down):
    context = lax.map(lambda triple: attend(triple[0], triple[1], triple[2]), (query, keys, values))
    hidden = (residual.astype(jnp.float32) + context).astype(jnp.bfloat16)
    token_total = SEQS * LENGTH
    hidden_flat = hidden.reshape(token_total, D)
    picked = routes.reshape(token_total * TOP).astype(jnp.int32)
    most_rows = CAP * N_EXPERT * N_TENSOR
    block_count = GROUPS
    block_width = FF // block_count

    def expert_pass(expert_id, outputs):
        matches = jnp.nonzero(picked == expert_id, size=most_rows, fill_value=token_total * TOP)[0].astype(jnp.int32)
        safe_index = jnp.minimum(matches, token_total * TOP - 1)
        token_rows = hidden_flat[safe_index // TOP]
        gate_part = jnp.dot(token_rows, w_gate[expert_id], preferred_element_type=jnp.float32)
        up_part = jnp.dot(token_rows, w_up[expert_id], preferred_element_type=jnp.float32)
        inner_rows = (jax.nn.silu(gate_part) * up_part).astype(jnp.bfloat16)
        down_full = w_down[expert_id]

        def add_block(block_id, running):
            inner_block = lax.dynamic_slice_in_dim(inner_rows, block_id * block_width, block_width, 1)
            down_block = lax.dynamic_slice_in_dim(down_full, block_id * block_width, block_width, 0)
            partial_value = jnp.dot(inner_block, down_block, preferred_element_type=jnp.float32).astype(jnp.bfloat16)
            return running + partial_value.astype(jnp.float32)
        summed = lax.fori_loop(0, block_count, add_block, jnp.zeros((most_rows, D), jnp.float32))
        return outputs.at[matches].set(summed.astype(jnp.bfloat16), mode='drop')
    expert_out = lax.fori_loop(0, EXPERTS, expert_pass, jnp.zeros((token_total * TOP, D), jnp.bfloat16))
    weighted = gates.reshape(token_total, TOP, 1).astype(jnp.float32) * expert_out.reshape(token_total, TOP, D).astype(jnp.float32)
    layer_out = hidden_flat.astype(jnp.float32) + lax.optimization_barrier(jnp.sum(weighted, axis=1))
    return layer_out.astype(jnp.bfloat16).reshape(SEQS, LENGTH, D)
```

```python
import math

import jax
import jax.numpy as jnp
from jax import lax
from jax.experimental import pallas as pl
from jax.experimental.pallas import tpu as pltpu
from jax.sharding import PartitionSpec as P

HD = 128
EXPERTS = 8
NZ = 8
SLOTS = 8
MAIN = 2 * SLOTS * EXPERTS
ROWS = MAIN + EXPERTS
CHUNKS = 4
MESH = pl.DeviceIdType.MESH
BF = jnp.bfloat16
F32 = jnp.float32


def dot(a, b):
    return jnp.dot(a, b, preferred_element_type=F32)


def copy_to(src, dst, send, recv, device):
    return pltpu.make_async_remote_copy(
        src_ref=src, dst_ref=dst, send_sem=send, recv_sem=recv, device_id=device, device_id_type=MESH
    )


def moe_kernel(
    hid, pm, po, gm, go, wg_any, wu_any, wd_any, out,
    wg, wu, wd, pk, pov, xr, ovr, xm, xp, inner, yps, ypr, ys, rr, fr, fov, ret, retov,
    w_sem, d_s, d_r, o_s, o_r, ag_s, ag_r, xs, xrs, yss, yrs, rs_s, rs_r, b_s, b_r, bo_s, bo_r,
):
    s, e, t = lax.axis_index("section"), lax.axis_index("expert"), lax.axis_index("tensor")
    z, c = t // 2, t % 2
    half = hid.shape[1]
    cw = half // CHUNKS
    barrier = pltpu.get_barrier_semaphore()
    for i in range(1, 32):
        other = (s * 2 + c) ^ (i % 4)
        pl.semaphore_signal(
            barrier, inc=1, device_id=(other // 2, (e + i // 4) % 8, z * 2 + other % 2), device_id_type=MESH
        )
    up, down = (z + 1) % NZ, (z + NZ - 1) % NZ
    for near in (up, down):
        pl.semaphore_signal(barrier, inc=1, device_id=(s, e, near * 2 + c), device_id_type=MESH)
    loads = []
    for part in range(2):
        h = (c + part) % 2
        rows = pl.ds(pl.multiple_of(h * half, half), half)
        loads.append(pltpu.make_async_copy(wg_any.at[0, rows, :], wg.at[part], w_sem.at[part]))
        loads.append(pltpu.make_async_copy(wu_any.at[0, rows, :], wu.at[part], w_sem.at[2 + part]))
        loads.append(pltpu.make_async_copy(wd_any.at[0, :, rows], wd.at[part], w_sem.at[4 + part]))
    for load in loads:
        load.start()

    tokens = hid[...]
    pk[...] = dot(pm[...], tokens).astype(BF).reshape(pk.shape)
    extra = dot(po[...], tokens)
    for j in range(16):
        pov[:, j, :] = extra[:, 128 * j : 128 * (j + 1)]
    pl.semaphore_wait(barrier, 33)

    own = s == c
    sent = []
    for i in range(8):
        ed = (e + i) % 8
        main = []
        for k in range(2):
            sd = (s + k) % 2
            main.append(
                copy_to(pk.at[ed * 2 + sd], xr.at[e * 2 + c], d_s.at[i * 2 + k], d_r.at[e * 2 + c], (sd, ed, z * 2 + s))
            )
        over = copy_to(pov.at[ed], ovr.at[e], o_s.at[i], o_r.at[e], (c, ed, z * 2 + s))
        main[1].start()
        if i == 0:
            @pl.when(own)
            def _():
                xr[e * 2 + c] = pk[e * 2 + s]
                ovr[e] = pov[e]

            @pl.when(jnp.logical_not(own))
            def _():
                main[0].start()
                over.start()
            own_main, own_over = main[0], over
        else:
            main[0].start()
            over.start()
            sent += [main[0], over]
        sent.append(main[1])
    for i in range(8):
        ef = (e + 8 - i) % 8
        for k in range(2):
            cf = (c + k) % 2
            arrival = copy_to(pk.at[0], xr.at[ef * 2 + cf], d_s.at[0], d_r.at[ef * 2 + cf], (c, ef, z * 2 + cf))
            if i == 0 and k == 0:
                pl.when(jnp.logical_not(own))(arrival.wait_recv)
            else:
                arrival.wait_recv()
        arrival = copy_to(pov.at[0], ovr.at[ef], o_s.at[0], o_r.at[ef], (c, ef, z * 2 + s))
        if i == 0:
            pl.when(jnp.logical_not(own))(arrival.wait_recv)
        else:
            arrival.wait_recv()
    xm[7, :MAIN, :] = xr[...].reshape(MAIN, half)
    for j in range(16):
        xm[7, MAIN:, 128 * j : 128 * (j + 1)] = ovr[:, j, :].astype(BF)

    def slot(way, d):
        return 7 if d == 0 else 6 if d == 4 else 2 * (d - 1) + way

    def cols(j):
        return pl.ds(cw * j, cw)

    partner = (s, e, z * 2 + 1 - c)
    ring = ((s, e, up * 2 + c), (s, e, down * 2 + c))
    half_of = ((0, 1), (2, 3))
    gather, share = {}, {}
    for way in range(2):
        for d in range(4):
            for j in range(CHUNKS) if d < 3 else half_of[way]:
                n = d * 4 + j
                gather[way, d, j] = copy_to(
                    xm.at[slot(way, d), :, cols(j)], xm.at[slot(way, d + 1), :, cols(j)],
                    ag_s.at[way, n], ag_r.at[way, n], ring[way],
                )
    for k in range(8):
        share[k] = copy_to(xm.at[k], xp.at[k], xs.at[k], xrs.at[k], partner)
    trade = {
        g: copy_to(yps.at[pl.ds(2 * g - 2, 2)], ypr.at[pl.ds(2 * g - 2, 2)], yss.at[g - 1], yrs.at[g - 1], partner)
        for g in range(1, 5)
    }

    def hidden_units(g, first, last):
        def piece(k, carry):
            at = pl.ds(pl.multiple_of(k * 256, 256), 256)
            left = xm[2 * g - 2 : 2 * g].reshape(2 * ROWS, half)
            right = xp[2 * g - 2 : 2 * g].reshape(2 * ROWS, half)
            gate = dot(left, wg[0, :, at]) + dot(right, wg[1, :, at])
            lift = dot(left, wu[0, :, at]) + dot(right, wu[1, :, at])
            inner[pl.ds((2 * g - 2) * ROWS, 2 * ROWS), at] = (gate / (1.0 + jnp.exp(-gate)) * lift).astype(BF)
            return carry

        lax.fori_loop(first, last, piece, 0)

    def down_out(g):
        rows = inner[pl.ds((2 * g - 2) * ROWS, 2 * ROWS), :]

        def theirs(j, carry):
            at = pl.ds(pl.multiple_of(j * cw, cw), cw)
            yps[pl.ds(2 * g - 2, 2), :, at] = dot(rows, wd[1, :, at]).astype(BF).reshape(2, ROWS, cw)
            return carry

        lax.fori_loop(0, CHUNKS, theirs, 0)
        trade[g].start()

    def down_own(g):
        rows = inner[pl.ds((2 * g - 2) * ROWS, 2 * ROWS), :]
        trade[g].wait_recv()

        def mine(j, carry):
            at = pl.ds(pl.multiple_of(j * cw, cw), cw)
            both = dot(rows, wd[0, :, at]).reshape(2, ROWS, cw) + ypr[pl.ds(2 * g - 2, 2), :, at].astype(F32)
            ys[pl.ds(2 * g - 2, 2), :, at] = both.astype(BF)
            return carry

        lax.fori_loop(0, CHUNKS, mine, 0)

    for j in range(CHUNKS):
        gather[0, 0, j].start()
        gather[1, 0, j].start()
    share[7].start()
    for load in loads:
        load.wait()
    for d in range(1, 5):
        if d > 1:
            for way in range(2):
                share[slot(way, d - 1)].wait_recv()
        for j in range(CHUNKS):
            for way in range(2):
                if d < 4 or j in half_of[way]:
                    gather[way, d - 1, j].wait_recv()
                    if (way, d, j) in gather:
                        gather[way, d, j].start()
                if d < 4 and j == CHUNKS - 1:
                    share[slot(way, d)].start()
            if d in (2, 3) and j % 2 == 1:
                hidden_units(d - 1, j // 2, j // 2 + 1)
        if d == 4:
            share[6].start()
            hidden_units(3, 0, 2)
    down_out(3)
    down_own(3)

    reduce = {}
    for way in range(2):
        for d in range(1, 5):
            target = slot(1 - way, d)
            for j in range(CHUNKS) if d < 4 else half_of[way]:
                n = (d - 1) * 4 + j
                reduce[way, d, j] = copy_to(
                    ys.at[target, :, cols(j)], rr.at[way, d - 1, :, cols(j)],
                    rs_s.at[way, n], rs_r.at[way, n], ring[way],
                )

    def pass_on(way, d, j, add):
        if add:
            reduce[way, d + 1, j].wait_recv()
            k = slot(1 - way, d)
            total = ys[k, :, cols(j)].astype(F32) + rr[way, d, :, cols(j)].astype(F32)
            ys[k, :, cols(j)] = total.astype(BF)
        reduce[way, d, j].start()

    for n in range(2):
        for way in range(2):
            pass_on(way, 3, half_of[1 - way][n], False)
    share[6].wait_recv()
    share[7].wait_recv()
    hidden_units(4, 0, 2)
    down_out(4)
    down_own(4)
    for n in range(2):
        for way in range(2):
            pass_on(way, 4, half_of[way][n], False)
    down_out(2)
    for n in range(2):
        for way in range(2):
            pass_on(way, 3, half_of[way][n], True)
    down_own(2)
    down_out(1)
    for h in range(2):
        for n in range(2):
            for way in range(2):
                pass_on(way, 2, half_of[1 - way if h == 0 else way][n], True)
    down_own(1)
    for h in range(2):
        for n in range(2):
            for way in range(2):
                pass_on(way, 1, half_of[1 - way if h == 0 else way][n], True)

    for j in range(CHUNKS):
        for way in range(2):
            reduce[way, 1, j].wait_recv()
        total = (
            ys[7, :, cols(j)].astype(F32) + rr[0, 0, :, cols(j)].astype(F32) + rr[1, 0, :, cols(j)].astype(F32)
        ).astype(BF)
        fr[:, :, cols(j)] = total[:MAIN].reshape(2 * EXPERTS, SLOTS, cw)
        tail = total[MAIN:].astype(F32)
        for k in range(cw // 128):
            fov[:, j * (cw // 128) + k, :] = tail[:, 128 * k : 128 * (k + 1)]

    for i in range(8):
        ed = (e + i) % 8
        main = []
        for k in range(2):
            cd = (c + k) % 2
            main.append(
                copy_to(fr.at[ed * 2 + cd], ret.at[e * 2 + s], b_s.at[i * 2 + k], b_r.at[e * 2 + s], (c, ed, z * 2 + cd))
            )
        over = copy_to(fov.at[ed], retov.at[e], bo_s.at[i], bo_r.at[e], (c, ed, z * 2 + s))
        main[1].start()
        if i == 0:
            @pl.when(own)
            def _():
                ret[e * 2 + s] = fr[e * 2 + c]
                retov[e] = fov[e]

            @pl.when(jnp.logical_not(own))
            def _():
                main[0].start()
                over.start()
            back_main, back_over = main[0], over
        else:
            main[0].start()
            over.start()
            sent += [main[0], over]
        sent.append(main[1])
    for i in range(8):
        ef = (e + 8 - i) % 8
        for k in range(2):
            sf = (s + k) % 2
            arrival = copy_to(fr.at[0], ret.at[ef * 2 + sf], b_s.at[0], b_r.at[ef * 2 + sf], (sf, ef, z * 2 + s))
            if i == 0 and k == 0:
                pl.when(jnp.logical_not(own))(arrival.wait_recv)
            else:
                arrival.wait_recv()
        arrival = copy_to(fov.at[0], retov.at[ef], bo_s.at[0], bo_r.at[ef], (c, ef, z * 2 + s))
        if i == 0:
            pl.when(jnp.logical_not(own))(arrival.wait_recv)
        else:
            arrival.wait_recv()

    rows = ret[...].reshape(MAIN, half)
    total = hid[...].astype(F32)
    for weight, part in ((gm, rows), (go, jnp.concatenate([retov[:, j, :] for j in range(16)], axis=1).astype(BF))):
        high = weight[...].astype(BF)
        low = (weight[...] - high.astype(F32)).astype(BF)
        total = total + dot(high, part) + dot(low, part)
    out[...] = total.astype(BF)

    @pl.when(jnp.logical_not(own))
    def _():
        for copy in (own_main, own_over, back_main, back_over):
            copy.wait_send()
    for copy in sent:
        copy.wait_send()
    for table in (gather, share, trade, reduce):
        for copy in table.values():
            copy.wait_send()


def moe(hidden, pm, po, gm, go, w_gate, w_up, w_down):
    half = hidden.shape[1]
    units = w_gate.shape[2]
    vmem = pl.BlockSpec(memory_space=pltpu.VMEM)
    hbm = pl.BlockSpec(memory_space=pl.ANY)
    dma = pltpu.SemaphoreType.DMA
    return pl.pallas_call(
        moe_kernel,
        out_shape=jax.ShapeDtypeStruct(hidden.shape, BF),
        in_specs=[vmem] * 5 + [hbm] * 3,
        out_specs=vmem,
        scratch_shapes=[
            pltpu.VMEM((2, half, units), BF),
            pltpu.VMEM((2, half, units), BF),
            pltpu.VMEM((2, units, half), BF),
            pltpu.VMEM((16, SLOTS, half), BF),
            pltpu.VMEM((8, 16, 128), F32),
            pltpu.VMEM((16, SLOTS, half), BF),
            pltpu.VMEM((8, 16, 128), F32),
            pltpu.VMEM((8, ROWS, half), BF),
            pltpu.VMEM((8, ROWS, half), BF),
            pltpu.VMEM((8 * ROWS, units), BF),
            pltpu.VMEM((8, ROWS, half), BF),
            pltpu.VMEM((8, ROWS, half), BF),
            pltpu.VMEM((8, ROWS, half), BF),
            pltpu.VMEM((2, 4, ROWS, half), BF),
            pltpu.VMEM((16, SLOTS, half), BF),
            pltpu.VMEM((8, 16, 128), F32),
            pltpu.VMEM((16, SLOTS, half), BF),
            pltpu.VMEM((8, 16, 128), F32),
            dma((6,)), dma((16,)), dma((16,)), dma((8,)), dma((8,)),
            dma((2, 16)), dma((2, 16)), dma((8,)), dma((8,)), dma((4,)), dma((4,)),
            dma((2, 16)), dma((2, 16)), dma((16,)), dma((16,)), dma((8,)), dma((8,)),
        ],
        compiler_params=pltpu.CompilerParams(
            collective_id=1, has_side_effects=True, vmem_limit_bytes=60 * 1024 * 1024
        ),
        name="moe",
    )(hidden, pm, po, gm, go, w_gate, w_up, w_down)


def tables(picked, gates):
    hits = picked[:, :, None] == jnp.arange(EXPERTS)
    named = jnp.any(hits, axis=1)
    gate = jnp.sum(jnp.where(hits, gates[:, :, None], 0.0), axis=1)
    place = jnp.cumsum(named.astype(jnp.int32), axis=0) - named.astype(jnp.int32)
    tokens = picked.shape[0]
    main = named[:, :, None] & (place[:, :, None] == jnp.arange(2 * SLOTS))
    gm = jnp.where(main, gate[:, :, None], 0.0).reshape(tokens, MAIN)
    over = named & (place == 2 * SLOTS)
    go = jnp.where(over, gate, 0.0)
    return main.reshape(tokens, MAIN).T.astype(BF), over.T.astype(BF), gm, go


def on_device(query, keys, values, residual, routes, gates, w_gate, w_up, w_down):
    both = lax.all_gather(jnp.concatenate((keys, values), axis=0), "tensor", axis=1, tiled=True)
    key_all, value_all = both[0], both[1]
    token_count = query.shape[1]
    length = key_all.shape[0]
    half_width = query.shape[2]
    local_heads = half_width // HD
    local_kv = keys.shape[2] // HD
    groups = local_heads // local_kv
    queries = query[0].reshape(token_count, local_kv, groups, HD)
    key_heads = key_all.reshape(length, local_kv, HD)
    value_heads = value_all.reshape(length, local_kv, HD)
    scores = jnp.einsum(
        "qkgd,tkd->kgqt", queries, key_heads, preferred_element_type=F32
    ) / math.sqrt(HD)
    start_row = lax.axis_index("tensor") * token_count
    query_positions = start_row + jnp.arange(token_count)
    causal = query_positions[:, None] >= jnp.arange(length)[None, :]
    masked = jnp.where(causal, scores, -1e30)
    row_peak = jnp.max(masked, axis=-1, keepdims=True)
    exp_terms = jnp.where(causal, jnp.exp(masked - row_peak), 0.0)
    weights = (exp_terms / jnp.sum(exp_terms, axis=-1, keepdims=True)).astype(BF)
    context = jnp.einsum("kgqt,tkd->qkgd", weights, value_heads, preferred_element_type=F32)
    hidden = (residual[0].astype(F32) + context.reshape(token_count, half_width)).astype(BF)
    pm, po, gm, go = tables(routes[0], gates[0])
    return moe(hidden, pm, po, gm, go, w_gate, w_up, w_down)[None]


def solution(mesh):
    return jax.shard_map(
        on_device,
        mesh=mesh,
        in_specs=(
            P("expert", "tensor", "section"),
            P("expert", "tensor", "section"),
            P("expert", "tensor", "section"),
            P("expert", "tensor", "section"),
            P("expert", "tensor", None),
            P("expert", "tensor", None),
            P("expert", None, "tensor"),
            P("expert", None, "tensor"),
            P("expert", "tensor", None),
        ),
        out_specs=P("expert", "tensor", "section"),
        check_vma=False,
    )
```

```python
import math

import jax
import jax.numpy as jnp
from jax import lax
from jax.experimental import pallas as pl
from jax.experimental.pallas import tpu as pltpu
from jax.sharding import PartitionSpec as P

HD = 128
EXPERTS = 8
NZ = 8
SLOTS = 8
MAIN = 2 * SLOTS * EXPERTS
ROWS = MAIN + EXPERTS
CHUNKS = 4
MESH = pl.DeviceIdType.MESH
BF = jnp.bfloat16
F32 = jnp.float32


def dot(a, b):
    return jnp.dot(a, b, preferred_element_type=F32)


def copy_to(src, dst, send, recv, device):
    return pltpu.make_async_remote_copy(
        src_ref=src, dst_ref=dst, send_sem=send, recv_sem=recv, device_id=device, device_id_type=MESH
    )


def layer_kernel(
    q_any, k_any, v_any, res_any, routes, gates, wg_any, wu_any, wd_any, out,
    qv, res, kv, qs, top, mass, acc, hid, gm, go,
    wg, wu, wd, pk, pov, xr, ovr, xm, xp, inner, yps, ypr, ys, rr, fr, fov, ret, retov,
    in_sem, kg_s, kg_r, kx_s, kx_r,
    w_sem, d_s, d_r, o_s, o_r, ag_s, ag_r, xs, xrs, yss, yrs, rs_s, rs_r, b_s, b_r, bo_s, bo_r,
):
    s, e, t = lax.axis_index("section"), lax.axis_index("expert"), lax.axis_index("tensor")
    z, c = t // 2, t % 2
    tokens, half = hid.shape
    cw = half // CHUNKS
    own_in = [
        pltpu.make_async_copy(k_any.at[0], kv.at[7, 0, 0], in_sem.at[0]),
        pltpu.make_async_copy(v_any.at[0], kv.at[7, 0, 1], in_sem.at[1]),
        pltpu.make_async_copy(q_any.at[0], qv, in_sem.at[2]),
        pltpu.make_async_copy(res_any.at[0], res, in_sem.at[3]),
    ]
    for load in own_in:
        load.start()
    barrier = pltpu.get_barrier_semaphore()
    for i in range(1, 32):
        other = (s * 2 + c) ^ (i % 4)
        pl.semaphore_signal(
            barrier, inc=1, device_id=(other // 2, (e + i // 4) % 8, z * 2 + other % 2), device_id_type=MESH
        )
    up, down = (z + 1) % NZ, (z + NZ - 1) % NZ
    for near in (up, down):
        pl.semaphore_signal(barrier, inc=1, device_id=(s, e, near * 2 + c), device_id_type=MESH)
    loads = []
    for part in range(2):
        h = (c + part) % 2
        rows = pl.ds(pl.multiple_of(h * half, half), half)
        loads.append(pltpu.make_async_copy(wg_any.at[0, rows, :], wg.at[part], w_sem.at[part]))
        loads.append(pltpu.make_async_copy(wu_any.at[0, rows, :], wu.at[part], w_sem.at[2 + part]))
        loads.append(pltpu.make_async_copy(wd_any.at[0, :, rows], wd.at[part], w_sem.at[4 + part]))

    def slot(way, d):
        return 7 if d == 0 else 6 if d == 4 else 2 * (d - 1) + way

    partner = (s, e, z * 2 + 1 - c)
    ring = ((s, e, up * 2 + c), (s, e, down * 2 + c))
    spread, swap = {}, {}
    for way in range(2):
        for d in range(4):
            for j in range(2) if d < 3 else (way,):
                spread[way, d, j] = copy_to(
                    kv.at[slot(way, d), 0, j], kv.at[slot(way, d + 1), 0, j],
                    kg_s.at[way, 2 * d + j], kg_r.at[way, 2 * d + j], ring[way],
                )
    for k in range(8):
        for j in range(2):
            swap[k, j] = copy_to(kv.at[k, 0, j], kv.at[k, 1, j], kx_s.at[k, j], kx_r.at[k, j], partner)

    own_in[0].wait()
    own_in[1].wait()
    pl.semaphore_wait(barrier, 33)
    for j in range(2):
        for way in range(2):
            spread[way, 0, j].start()
        swap[7, j].start()
    for load in loads:
        load.start()

    lane = lax.broadcasted_iota(jnp.int32, (tokens, MAIN), 1)
    first, second = routes[0, :, 0:1], routes[0, :, 1:2]
    gate0, gate1 = gates[0, :, 0:1], gates[0, :, 1:2]
    earlier = (
        lax.broadcasted_iota(jnp.int32, (tokens, tokens), 0) > lax.broadcasted_iota(jnp.int32, (tokens, tokens), 1)
    ).astype(BF)

    def placed(expert, wanted):
        is0, is1 = first == expert, second == expert
        named = jnp.where(is0 | is1, 1.0, 0.0)
        place = dot(earlier, named.astype(BF))
        hit = jnp.where(place == wanted.astype(F32), named, 0.0)
        return hit, hit * (jnp.where(is0, gate0, 0.0) + jnp.where(is1, gate1, 0.0))

    hit_main, gm[...] = placed(lane // (2 * SLOTS), lane % (2 * SLOTS))
    few = lax.broadcasted_iota(jnp.int32, (tokens, EXPERTS), 1)
    hit_over, go[...] = placed(few, jnp.full_like(few, 2 * SLOTS))

    own_in[2].wait()
    kv_heads = qs.shape[0]
    group = qs.shape[1] // tokens
    for h in range(kv_heads):
        for g in range(group):
            qs[h, tokens * g : tokens * (g + 1), :] = qv[:, HD * (h * group + g) : HD * (h * group + g + 1)]
    stacked = group * tokens
    scale = 1.0 / math.sqrt(HD)

    def attend(start, count, bias, fresh):
        keys = count * 2 * tokens

        def head(h, carry):
            at = pl.ds(pl.multiple_of(h * HD, HD), HD)
            k = kv[start : start + count, :, 0, :, at].reshape(keys, HD)
            v = kv[start : start + count, :, 1, :, at].reshape(keys, HD)
            scores = lax.dot_general(qs[h], k, (((1,), (1,)), ((), ())), preferred_element_type=F32) * scale + bias
            peak = jnp.max(scores, axis=1, keepdims=True)
            if not fresh:
                peak = jnp.maximum(peak, top[h])
            terms = jnp.exp(scores - peak)
            total = jnp.sum(terms, axis=1, keepdims=True)
            context = dot(terms.astype(BF), v)
            if not fresh:
                fade = jnp.exp(top[h] - peak)
                total = total + mass[h] * fade
                context = context + acc[h] * fade
            top[h], mass[h], acc[h] = peak, total, context
            return carry

        lax.fori_loop(0, kv_heads, head, 0)

    for j in range(2):
        swap[7, j].wait_recv()
    row = lax.broadcasted_iota(jnp.int32, (stacked, 2 * tokens), 0) % tokens
    col = lax.broadcasted_iota(jnp.int32, (stacked, 2 * tokens), 1)
    attend(7, 1, jnp.where(col <= jnp.where(col < tokens, row, jnp.where(c == 1, 2 * tokens, -1)), 0.0, -1e30), True)

    def ring_bias(d):
        col = lax.broadcasted_iota(jnp.int32, (1, (2 if d < 4 else 1) * 2 * tokens), 1)
        return jnp.where(jnp.where(col < 2 * tokens, z - d, z + d - NZ) >= 0, 0.0, -1e30)

    for d in range(1, 5):
        for j in range(2):
            for way in range(2) if d < 4 else (j,):
                spread[way, d - 1, j].wait_recv()
                if (way, d, j) in spread:
                    spread[way, d, j].start()
                swap[slot(way, d), j].start()
        if d > 1:
            for way in range(2):
                for j in range(2):
                    swap[slot(way, d - 1), j].wait_recv()
            attend(slot(0, d - 1), 2, ring_bias(d - 1), False)
    for j in range(2):
        swap[6, j].wait_recv()
    attend(6, 1, ring_bias(4), False)
    own_in[3].wait()
    for h in range(kv_heads):
        context = acc[h] / mass[h]
        for g in range(group):
            at = slice(HD * (h * group + g), HD * (h * group + g + 1))
            hid[:, at] = (res[:, at].astype(F32) + context[tokens * g : tokens * (g + 1), :]).astype(BF)

    packed = hid[...]
    dims = (((0,), (0,)), ((), ()))
    pk[...] = lax.dot_general(hit_main.astype(BF), packed, dims, preferred_element_type=F32).astype(BF).reshape(pk.shape)
    extra = lax.dot_general(hit_over.astype(BF), packed, dims, preferred_element_type=F32)
    for j in range(16):
        pov[:, j, :] = extra[:, 128 * j : 128 * (j + 1)]

    own = s == c
    sent = []
    for i in range(8):
        ed = (e + i) % 8
        main = []
        for k in range(2):
            sd = (s + k) % 2
            main.append(
                copy_to(pk.at[ed * 2 + sd], xr.at[e * 2 + c], d_s.at[i * 2 + k], d_r.at[e * 2 + c], (sd, ed, z * 2 + s))
            )
        over = copy_to(pov.at[ed], ovr.at[e], o_s.at[i], o_r.at[e], (c, ed, z * 2 + s))
        main[1].start()
        if i == 0:
            @pl.when(own)
            def _():
                xr[e * 2 + c] = pk[e * 2 + s]
                ovr[e] = pov[e]

            @pl.when(jnp.logical_not(own))
            def _():
                main[0].start()
                over.start()
            own_main, own_over = main[0], over
        else:
            main[0].start()
            over.start()
            sent += [main[0], over]
        sent.append(main[1])
    for i in range(8):
        ef = (e + 8 - i) % 8
        for k in range(2):
            cf = (c + k) % 2
            arrival = copy_to(pk.at[0], xr.at[ef * 2 + cf], d_s.at[0], d_r.at[ef * 2 + cf], (c, ef, z * 2 + cf))
            if i == 0 and k == 0:
                pl.when(jnp.logical_not(own))(arrival.wait_recv)
            else:
                arrival.wait_recv()
        arrival = copy_to(pov.at[0], ovr.at[ef], o_s.at[0], o_r.at[ef], (c, ef, z * 2 + s))
        if i == 0:
            pl.when(jnp.logical_not(own))(arrival.wait_recv)
        else:
            arrival.wait_recv()
    xm[7, :MAIN, :] = xr[...].reshape(MAIN, half)
    for j in range(16):
        xm[7, MAIN:, 128 * j : 128 * (j + 1)] = ovr[:, j, :].astype(BF)

    def cols(j):
        return pl.ds(cw * j, cw)

    half_of = ((0, 1), (2, 3))
    gather, share = {}, {}
    for way in range(2):
        for d in range(4):
            for j in range(CHUNKS) if d < 3 else half_of[way]:
                n = d * 4 + j
                gather[way, d, j] = copy_to(
                    xm.at[slot(way, d), :, cols(j)], xm.at[slot(way, d + 1), :, cols(j)],
                    ag_s.at[way, n], ag_r.at[way, n], ring[way],
                )
    for k in range(8):
        share[k] = copy_to(xm.at[k], xp.at[k], xs.at[k], xrs.at[k], partner)
    trade = {
        g: copy_to(yps.at[pl.ds(2 * g - 2, 2)], ypr.at[pl.ds(2 * g - 2, 2)], yss.at[g - 1], yrs.at[g - 1], partner)
        for g in range(1, 5)
    }

    def hidden_units(g, first, last):
        def piece(k, carry):
            at = pl.ds(pl.multiple_of(k * 256, 256), 256)
            left = xm[2 * g - 2 : 2 * g].reshape(2 * ROWS, half)
            right = xp[2 * g - 2 : 2 * g].reshape(2 * ROWS, half)
            gate = dot(left, wg[0, :, at]) + dot(right, wg[1, :, at])
            lift = dot(left, wu[0, :, at]) + dot(right, wu[1, :, at])
            inner[pl.ds((2 * g - 2) * ROWS, 2 * ROWS), at] = (gate / (1.0 + jnp.exp(-gate)) * lift).astype(BF)
            return carry

        lax.fori_loop(first, last, piece, 0)

    def down_out(g):
        rows = inner[pl.ds((2 * g - 2) * ROWS, 2 * ROWS), :]

        def theirs(j, carry):
            at = pl.ds(pl.multiple_of(j * cw, cw), cw)
            yps[pl.ds(2 * g - 2, 2), :, at] = dot(rows, wd[1, :, at]).astype(BF).reshape(2, ROWS, cw)
            return carry

        lax.fori_loop(0, CHUNKS, theirs, 0)
        trade[g].start()

    def down_own(g):
        rows = inner[pl.ds((2 * g - 2) * ROWS, 2 * ROWS), :]
        trade[g].wait_recv()

        def mine(j, carry):
            at = pl.ds(pl.multiple_of(j * cw, cw), cw)
            both = dot(rows, wd[0, :, at]).reshape(2, ROWS, cw) + ypr[pl.ds(2 * g - 2, 2), :, at].astype(F32)
            ys[pl.ds(2 * g - 2, 2), :, at] = both.astype(BF)
            return carry

        lax.fori_loop(0, CHUNKS, mine, 0)

    for j in range(CHUNKS):
        gather[0, 0, j].start()
        gather[1, 0, j].start()
    share[7].start()
    for load in loads:
        load.wait()
    for d in range(1, 5):
        if d > 1:
            for way in range(2):
                share[slot(way, d - 1)].wait_recv()
        for j in range(CHUNKS):
            for way in range(2):
                if d < 4 or j in half_of[way]:
                    gather[way, d - 1, j].wait_recv()
                    if (way, d, j) in gather:
                        gather[way, d, j].start()
                if d < 4 and j == CHUNKS - 1:
                    share[slot(way, d)].start()
            if d in (2, 3) and j % 2 == 1:
                hidden_units(d - 1, j // 2, j // 2 + 1)
        if d == 4:
            share[6].start()
            hidden_units(3, 0, 2)
    down_out(3)
    down_own(3)

    reduce = {}
    for way in range(2):
        for d in range(1, 5):
            target = slot(1 - way, d)
            for j in range(CHUNKS) if d < 4 else half_of[way]:
                n = (d - 1) * 4 + j
                reduce[way, d, j] = copy_to(
                    ys.at[target, :, cols(j)], rr.at[way, d - 1, :, cols(j)],
                    rs_s.at[way, n], rs_r.at[way, n], ring[way],
                )

    def pass_on(way, d, j, add):
        if add:
            reduce[way, d + 1, j].wait_recv()
            k = slot(1 - way, d)
            total = ys[k, :, cols(j)].astype(F32) + rr[way, d, :, cols(j)].astype(F32)
            ys[k, :, cols(j)] = total.astype(BF)
        reduce[way, d, j].start()

    for n in range(2):
        for way in range(2):
            pass_on(way, 3, half_of[1 - way][n], False)
    share[6].wait_recv()
    share[7].wait_recv()
    hidden_units(4, 0, 2)
    down_out(4)
    down_own(4)
    for n in range(2):
        for way in range(2):
            pass_on(way, 4, half_of[way][n], False)
    down_out(2)
    for n in range(2):
        for way in range(2):
            pass_on(way, 3, half_of[way][n], True)
    down_own(2)
    down_out(1)
    for h in range(2):
        for n in range(2):
            for way in range(2):
                pass_on(way, 2, half_of[1 - way if h == 0 else way][n], True)
    down_own(1)
    for h in range(2):
        for n in range(2):
            for way in range(2):
                pass_on(way, 1, half_of[1 - way if h == 0 else way][n], True)

    for j in range(CHUNKS):
        for way in range(2):
            reduce[way, 1, j].wait_recv()
        total = (
            ys[7, :, cols(j)].astype(F32) + rr[0, 0, :, cols(j)].astype(F32) + rr[1, 0, :, cols(j)].astype(F32)
        ).astype(BF)
        fr[:, :, cols(j)] = total[:MAIN].reshape(2 * EXPERTS, SLOTS, cw)
        tail = total[MAIN:].astype(F32)
        for k in range(cw // 128):
            fov[:, j * (cw // 128) + k, :] = tail[:, 128 * k : 128 * (k + 1)]

    for i in range(8):
        ed = (e + i) % 8
        main = []
        for k in range(2):
            cd = (c + k) % 2
            main.append(
                copy_to(fr.at[ed * 2 + cd], ret.at[e * 2 + s], b_s.at[i * 2 + k], b_r.at[e * 2 + s], (c, ed, z * 2 + cd))
            )
        over = copy_to(fov.at[ed], retov.at[e], bo_s.at[i], bo_r.at[e], (c, ed, z * 2 + s))
        main[1].start()
        if i == 0:
            @pl.when(own)
            def _():
                ret[e * 2 + s] = fr[e * 2 + c]
                retov[e] = fov[e]

            @pl.when(jnp.logical_not(own))
            def _():
                main[0].start()
                over.start()
            back_main, back_over = main[0], over
        else:
            main[0].start()
            over.start()
            sent += [main[0], over]
        sent.append(main[1])
    for i in range(8):
        ef = (e + 8 - i) % 8
        for k in range(2):
            sf = (s + k) % 2
            arrival = copy_to(fr.at[0], ret.at[ef * 2 + sf], b_s.at[0], b_r.at[ef * 2 + sf], (sf, ef, z * 2 + s))
            if i == 0 and k == 0:
                pl.when(jnp.logical_not(own))(arrival.wait_recv)
            else:
                arrival.wait_recv()
        arrival = copy_to(fov.at[0], retov.at[ef], bo_s.at[0], bo_r.at[ef], (c, ef, z * 2 + s))
        if i == 0:
            pl.when(jnp.logical_not(own))(arrival.wait_recv)
        else:
            arrival.wait_recv()

    rows = ret[...].reshape(MAIN, half)
    total = hid[...].astype(F32)
    for weight, part in ((gm, rows), (go, jnp.concatenate([retov[:, j, :] for j in range(16)], axis=1).astype(BF))):
        high = weight[...].astype(BF)
        low = (weight[...] - high.astype(F32)).astype(BF)
        total = total + dot(high, part) + dot(low, part)
    out[0] = total.astype(BF)

    @pl.when(jnp.logical_not(own))
    def _():
        for copy in (own_main, own_over, back_main, back_over):
            copy.wait_send()
    for copy in sent:
        copy.wait_send()
    for table in (spread, swap, gather, share, trade, reduce):
        for copy in table.values():
            copy.wait_send()


def on_device(query, keys, values, residual, routes, gates, w_gate, w_up, w_down):
    _, tokens, half = query.shape
    units = w_gate.shape[2]
    kv_heads = keys.shape[2] // HD
    stacked = half // HD // kv_heads * tokens
    vmem = pl.BlockSpec(memory_space=pltpu.VMEM)
    hbm = pl.BlockSpec(memory_space=pl.ANY)
    dma = pltpu.SemaphoreType.DMA
    return pl.pallas_call(
        layer_kernel,
        out_shape=jax.ShapeDtypeStruct(query.shape, BF),
        in_specs=[hbm] * 4 + [vmem] * 2 + [hbm] * 3,
        out_specs=vmem,
        scratch_shapes=[
            pltpu.VMEM((tokens, half), BF),
            pltpu.VMEM((tokens, half), BF),
            pltpu.VMEM((8, 2, 2, tokens, kv_heads * HD), BF),
            pltpu.VMEM((kv_heads, stacked, HD), BF),
            pltpu.VMEM((kv_heads, stacked, 1), F32),
            pltpu.VMEM((kv_heads, stacked, 1), F32),
            pltpu.VMEM((kv_heads, stacked, HD), F32),
            pltpu.VMEM((tokens, half), BF),
            pltpu.VMEM((tokens, MAIN), F32),
            pltpu.VMEM((tokens, EXPERTS), F32),
            pltpu.VMEM((2, half, units), BF),
            pltpu.VMEM((2, half, units), BF),
            pltpu.VMEM((2, units, half), BF),
            pltpu.VMEM((16, SLOTS, half), BF),
            pltpu.VMEM((8, 16, 128), F32),
            pltpu.VMEM((16, SLOTS, half), BF),
            pltpu.VMEM((8, 16, 128), F32),
            pltpu.VMEM((8, ROWS, half), BF),
            pltpu.VMEM((8, ROWS, half), BF),
            pltpu.VMEM((8 * ROWS, units), BF),
            pltpu.VMEM((8, ROWS, half), BF),
            pltpu.VMEM((8, ROWS, half), BF),
            pltpu.VMEM((8, ROWS, half), BF),
            pltpu.VMEM((2, 4, ROWS, half), BF),
            pltpu.VMEM((16, SLOTS, half), BF),
            pltpu.VMEM((8, 16, 128), F32),
            pltpu.VMEM((16, SLOTS, half), BF),
            pltpu.VMEM((8, 16, 128), F32),
            dma((4,)), dma((2, 8)), dma((2, 8)), dma((8, 2)), dma((8, 2)),
            dma((6,)), dma((16,)), dma((16,)), dma((8,)), dma((8,)),
            dma((2, 16)), dma((2, 16)), dma((8,)), dma((8,)), dma((4,)), dma((4,)),
            dma((2, 16)), dma((2, 16)), dma((16,)), dma((16,)), dma((8,)), dma((8,)),
        ],
        compiler_params=pltpu.CompilerParams(
            collective_id=1, has_side_effects=True, vmem_limit_bytes=60 * 1024 * 1024
        ),
        name="layer",
    )(query, keys, values, residual, routes, gates, w_gate, w_up, w_down)


def solution(mesh):
    return jax.shard_map(
        on_device,
        mesh=mesh,
        in_specs=(
            P("expert", "tensor", "section"),
            P("expert", "tensor", "section"),
            P("expert", "tensor", "section"),
            P("expert", "tensor", "section"),
            P("expert", "tensor", None),
            P("expert", "tensor", None),
            P("expert", None, "tensor"),
            P("expert", None, "tensor"),
            P("expert", "tensor", None),
        ),
        out_specs=P("expert", "tensor", "section"),
        check_vma=False,
    )
```

```python
import math

import jax
import jax.numpy as jnp
from jax import lax
from jax.experimental import pallas as pl
from jax.experimental.pallas import tpu as pltpu
from jax.sharding import PartitionSpec as P

HD = 128
EXPERTS = 8
NZ = 8
SLOTS = 8
MAIN = 2 * SLOTS * EXPERTS
ROWS = MAIN + EXPERTS
CHUNKS = 4
WIDE = 768
RING = 256
FAR = (0, 2, 4, 6, 5, 3, 1)
MESH = pl.DeviceIdType.MESH
BF = jnp.bfloat16
F32 = jnp.float32


def dot(a, b):
    return jnp.dot(a, b, preferred_element_type=F32)


def dot_rows(a, b):
    return lax.dot_general(a, b, (((0,), (0,)), ((), ())), preferred_element_type=F32)


def copy_to(src, dst, send, recv, device):
    return pltpu.make_async_remote_copy(
        src_ref=src, dst_ref=dst, send_sem=send, recv_sem=recv, device_id=device, device_id_type=MESH
    )


def layer_kernel(
    q_any, k_any, v_any, res_any, routes, gates, wg_any, wu_any, wd_any, out,
    qv, res, kv, qs, top, mass, acc, hid, rz, hits, overs, high, low, ohigh, olow, hz,
    wg, wu, wd, pk, pov, ovr, pw, pvw, ovw, xm, xp, partial, inner, yps, ypr, ys, rr, fov, ret, retov,
    rb, pvb, ovb, cz, rc,
    in_sem, rz_s, rz_r, kg_s, kg_r, kx_s, kx_r, hz_s, hz_r, dw_s, dw_r, ow_s, ow_r,
    w_sem, d_s, d_r, o_s, o_r, ag_s, ag_r, xs, xrs, yss, yrs, rs_s, rs_r, b_s, b_r, bo_s, bo_r,
    bw_s, bw_r, vw_s, vw_r, cr_s, cr_r,
):
    s, e, t = lax.axis_index("section"), lax.axis_index("expert"), lax.axis_index("tensor")
    z, c = t // 2, t % 2
    tokens, half = hid.shape
    cw = half // CHUNKS
    kv_heads = qs.shape[0]
    own_in = []
    for h in range(kv_heads):
        at = pl.ds(HD * h, HD)
        own_in.append(pltpu.make_async_copy(k_any.at[0, :, at], kv.at[7, 0, h, 0], in_sem.at[2 * h]))
        own_in.append(pltpu.make_async_copy(v_any.at[0, :, at], kv.at[7, 0, h, 1], in_sem.at[2 * h + 1]))
    queries_in = pltpu.make_async_copy(q_any.at[0], qv, in_sem.at[8])
    residual_in = pltpu.make_async_copy(res_any.at[0], res, in_sem.at[9])
    own_in += [queries_in, residual_in]
    for load in own_in:
        load.start()
    barrier = pltpu.get_barrier_semaphore()
    for i in range(1, 32):
        other = (s * 2 + c) ^ (i % 4)
        pl.semaphore_signal(
            barrier, inc=1, device_id=(other // 2, (e + i // 4) % 8, z * 2 + other % 2), device_id_type=MESH
        )
    up, down = (z + 1) % NZ, (z + NZ - 1) % NZ
    for k in range(1, NZ):
        pl.semaphore_signal(barrier, inc=1, device_id=(s, e, ((z + k) % NZ) * 2 + c), device_id_type=MESH)
    rz[7] = jnp.zeros(rz.shape[1:], F32)
    rz[7, 0:2, 0:tokens] = routes[...].astype(F32)
    rz[7, 2:4, 0:tokens] = gates[...]
    loads = []
    for part in range(2):
        h = (c + part) % 2
        rows = pl.ds(pl.multiple_of(h * half, half), half)
        loads.append(pltpu.make_async_copy(wg_any.at[0, rows, :], wg.at[part], w_sem.at[part]))
        loads.append(pltpu.make_async_copy(wu_any.at[0, rows, :], wu.at[part], w_sem.at[2 + part]))
        loads.append(pltpu.make_async_copy(wd_any.at[0, :, rows], wd.at[part], w_sem.at[4 + part]))

    def slot(way, d):
        return 7 if d == 0 else 6 if d == 4 else 2 * (d - 1) + way

    partner = (s, e, z * 2 + 1 - c)
    ring = ((s, e, up * 2 + c), (s, e, down * 2 + c))

    def spread(way, d, h):
        return copy_to(
            kv.at[slot(way, d), 0, h], kv.at[slot(way, d + 1), 0, h],
            kg_s.at[way, 4 * d + h], kg_r.at[way, 4 * d + h], ring[way],
        )

    def swap(k, h):
        return copy_to(kv.at[k, 0, h], kv.at[k, 1, h], kx_s.at[k, h], kx_r.at[k, h], partner)

    tell = [
        copy_to(rz.at[7], rz.at[FAR[k - 1]], rz_s.at[k - 1], rz_r.at[k - 1], (s, e, ((z + k) % NZ) * 2 + c))
        for k in range(1, NZ)
    ]
    for load in own_in[:8]:
        load.wait()
    pl.semaphore_wait(barrier, 38)
    for h in range(kv_heads):
        for way in range(2):
            spread(way, 0, h).start()
        swap(7, h).start()
    for copy in tell:
        copy.start()
    for load in loads:
        load.start()

    earlier = (
        lax.broadcasted_iota(jnp.int32, (tokens, tokens), 0) < lax.broadcasted_iota(jnp.int32, (tokens, tokens), 1)
    ).astype(BF)

    line = lax.broadcasted_iota(jnp.int32, (MAIN, tokens), 0)
    few = lax.broadcasted_iota(jnp.int32, (EXPERTS, tokens), 0)

    def placed(k, expert, wanted, hit_ref, high_ref, low_ref):
        is0, is1 = (rz[k, n : n + 1, 0:tokens] == expert.astype(F32) for n in range(2))
        gate0, gate1 = (rz[k, n : n + 1, 0:tokens] for n in (2, 3))
        named = jnp.where(is0 | is1, 1.0, 0.0)
        place = dot(named.astype(BF), earlier)
        hit = jnp.where(place == wanted.astype(F32), named, 0.0)
        weight = hit * (jnp.where(is0, gate0, 0.0) + jnp.where(is1, gate1, 0.0))
        top_part = weight.astype(BF)
        hit_ref[k] = hit.astype(BF)
        high_ref[k] = top_part
        low_ref[k] = (weight - top_part.astype(F32)).astype(BF)

    def slot_tables(k):
        placed(k, line // (2 * SLOTS), line % (2 * SLOTS), hits, high, low)
        placed(k, few, jnp.full_like(few, 2 * SLOTS), overs, ohigh, olow)

    slot_tables(7)
    queries_in.wait()
    group = qs.shape[1] // tokens
    for h in range(kv_heads):
        for g in range(group):
            qs[h, tokens * g : tokens * (g + 1), :] = qv[:, HD * (h * group + g) : HD * (h * group + g + 1)]
    stacked = group * tokens
    scale = math.log2(math.e) / math.sqrt(HD)

    def attend(start, count, bias, fresh, h):
        keys = count * 2 * tokens
        k = kv[start : start + count, :, h, 0].reshape(keys, HD)
        v = kv[start : start + count, :, h, 1].reshape(keys, HD)
        scores = lax.dot_general(qs[h], k, (((1,), (1,)), ((), ())), preferred_element_type=F32) * scale + bias
        peak = jnp.max(scores, axis=1, keepdims=True)
        if not fresh:
            peak = jnp.maximum(peak, top[h])
        terms = jnp.exp2(scores - peak).astype(BF)
        both = dot(terms, jnp.concatenate([v, jnp.ones_like(v)], axis=1))
        context, total = both[:, :HD], both[:, HD:]
        if not fresh:
            fade = jnp.exp2(top[h] - peak)
            total = total + mass[h] * fade
            context = context + acc[h] * fade
        top[h], mass[h], acc[h] = peak, total, context

    row = lax.broadcasted_iota(jnp.int32, (stacked, 2 * tokens), 0) % tokens
    col = lax.broadcasted_iota(jnp.int32, (stacked, 2 * tokens), 1)
    diagonal = jnp.where(col <= jnp.where(col < tokens, row, jnp.where(c == 1, 2 * tokens, -1)), 0.0, -1e30)

    def ring_bias(d):
        col = lax.broadcasted_iota(jnp.int32, (1, (2 if d < 4 else 1) * 2 * tokens), 1)
        return jnp.where(jnp.where(col < 2 * tokens, z - d, z + d - NZ) >= 0, 0.0, -1e30)

    def first_step(h, carry):
        swap(7, h).wait_recv()
        attend(7, 1, diagonal, True, h)
        return carry

    lax.fori_loop(0, kv_heads, first_step, 0)
    for d in range(1, 4):
        bias = ring_bias(d - 1) if d > 1 else None

        def ring_step(h, carry, d=d, bias=bias):
            for way in range(2):
                spread(way, d - 1, h).wait_recv()
                if d < 3:
                    spread(way, d, h).start()
                else:
                    pl.when(h // 2 == way)(spread(way, d, h).start)
                swap(slot(way, d), h).start()
            if d > 1:
                for way in range(2):
                    swap(slot(way, d - 1), h).wait_recv()
                attend(slot(0, d - 1), 2, bias, False, h)
            return carry

        lax.fori_loop(0, kv_heads, ring_step, 0)
    bias = ring_bias(3)

    def last_step(h, carry):
        for way in range(2):
            swap(slot(way, 3), h).wait_recv()
        attend(slot(0, 3), 2, bias, False, h)
        return carry

    bias4 = ring_bias(4)
    for copy in tell:
        copy.wait_recv()
    for k in range(7):
        slot_tables(k)
    for h in range(2):
        last_step(h, 0)
        for way in range(2):
            spread(way, 3, 2 * way + h).wait_recv()
            swap(6, 2 * way + h).start()
    residual_in.wait()

    own = s == c
    wide = WIDE
    rings = (half - wide) // RING
    ring_half = (tuple(range((rings + 1) // 2)), tuple(range((rings + 1) // 2, rings)))
    hw = half // kv_heads
    sent, own_sent = [], []

    def ring_cols(j):
        return pl.ds(wide + RING * j, RING)

    def send(copy, i, same):
        if i == 0 and same:
            pl.when(jnp.logical_not(own))(copy.start)
            own_sent.append(copy)
        else:
            copy.start()
            sent.append(copy)

    def receive(copy, i, same):
        if i == 0 and same:
            pl.when(jnp.logical_not(own))(copy.wait_recv)
        else:
            copy.wait_recv()

    def source_rows(ef, cf):
        return pl.ds(pl.multiple_of((ef * 2 + cf) * SLOTS, SLOTS), SLOTS)

    carry_on = {}
    for way in range(2):
        for d in range(4):
            for j in range(2) if d < 3 else (way,):
                at = pl.ds(wide // 2 * j, wide // 2)
                carry_on[way, d, j] = copy_to(
                    hz.at[slot(way, d), :, at], hz.at[slot(way, d + 1), :, at],
                    hz_s.at[way, 2 * d + j], hz_r.at[way, 2 * d + j], ring[way],
                )

    for h in range(kv_heads):
        swap(6, h).wait_recv()
        if h >= 2:
            last_step(h, 0)
        attend(6, 1, bias4, False, h)
        context = acc[h] / mass[h]
        for g in range(group):
            at = slice(HD * (h * group + g), HD * (h * group + g + 1))
            hid[:, at] = (res[:, at].astype(F32) + context[tokens * g : tokens * (g + 1), :]).astype(BF)
        from_col = hw * h
        if from_col < wide:
            to_col = min(wide, from_col + hw)
            hz[7, :, from_col:to_col] = hid[:, from_col:to_col]
            for j in range(2):
                if from_col < wide // 2 * (j + 1) <= to_col:
                    for way in range(2):
                        carry_on[way, 0, j].start()
        if h == 0:
            continue
        a = h - 1
        from_col = max(from_col, wide)
        width = hw * (h + 1) - from_col
        piece = hid[:, from_col : from_col + width]
        part = pl.ds(from_col - wide, width)
        pk[:, :, part] = dot(hits[7], piece).astype(BF).reshape(16, SLOTS, width)
        extra = dot(overs[7], piece)
        for q in range(width // 128):
            pov[a, :, q, :] = extra[:, 128 * q : 128 * (q + 1)]
        land = pl.ds(from_col, width)

        @pl.when(own)
        def _():
            xm[7, source_rows(e, c), land] = pk[e * 2 + s, :, part]
            ovr[a, e] = pov[a, e]

        for i in range(8):
            ed = (e + i) % 8
            for k in (1, 0):
                sd = (s + k) % 2
                send(
                    copy_to(
                        pk.at[ed * 2 + sd, :, part], xm.at[7, source_rows(e, c), land],
                        d_s.at[a, i * 2 + k], d_r.at[a, e * 2 + c], (sd, ed, z * 2 + s),
                    ), i, k == 0,
                )
            send(copy_to(pov.at[a, ed], ovr.at[a, e], o_s.at[a, i], o_r.at[a, e], (c, ed, z * 2 + s)), i, True)

    groups = ((7, 1), (0, 2), (2, 2), (4, 2), (6, 1))

    def send_wide(w):
        start, count = groups[w]
        for p in range(count):
            tokens_of = hz[start + p]
            pw[w, :, p] = dot(hits[start + p], tokens_of).astype(BF).reshape(16, SLOTS, wide)
            extra = dot(overs[start + p], tokens_of)
            for q in range(wide // 128):
                pvw[w, :, p, q, :] = extra[:, 128 * q : 128 * (q + 1)]
        many = pl.ds(0, count)
        slots = pl.ds(start, count)
        at = pl.ds(0, wide)

        @pl.when(own)
        def _():
            xm[slots, source_rows(e, c), at] = pw[w, e * 2 + s, many]
            ovw[w, e, many] = pvw[w, e, many]

        for i in range(8):
            ed = (e + i) % 8
            for k in (1, 0):
                sd = (s + k) % 2
                send(
                    copy_to(
                        pw.at[w, ed * 2 + sd, many], xm.at[slots, source_rows(e, c), at],
                        dw_s.at[w, i * 2 + k], dw_r.at[w, e * 2 + c], (sd, ed, z * 2 + s),
                    ), i, k == 0,
                )
            send(
                copy_to(pvw.at[w, ed, many], ovw.at[w, e, many], ow_s.at[w, i], ow_r.at[w, e], (c, ed, z * 2 + s)),
                i, True,
            )

    def receive_wide(w):
        start, count = groups[w]
        many = pl.ds(0, count)
        slots = pl.ds(start, count)
        at = pl.ds(0, wide)
        for i in range(8):
            ef = (e + 8 - i) % 8
            for k in range(2):
                cf = (c + k) % 2
                receive(
                    copy_to(
                        pw.at[w, 0, many], xm.at[slots, source_rows(ef, cf), at],
                        dw_s.at[w, 0], dw_r.at[w, ef * 2 + cf], (c, ef, z * 2 + cf),
                    ), i, k == 0,
                )
            receive(
                copy_to(pvw.at[w, 0, many], ovw.at[w, ef, many], ow_s.at[w, 0], ow_r.at[w, ef], (c, ef, z * 2 + s)),
                i, True,
            )
        for p in range(count):
            for q in range(wide // 128):
                xm[start + p, MAIN:, 128 * q : 128 * (q + 1)] = ovw[w, :, p, q, :].astype(BF)
            share[start + p, 0].start()

    def carry(d):
        for j in range(2):
            for way in range(2) if d < 4 else (j,):
                carry_on[way, d - 1, j].wait_recv()
                if (way, d, j) in carry_on:
                    carry_on[way, d, j].start()

    def cols(j):
        return pl.ds(cw * j, cw)

    half_of = ((0, 1), (2, 3))
    gather, share = {}, {}
    split = wide + 3 * RING
    parts = ((0, wide), (wide, split), (split, half))
    for way in range(2):
        for d in range(4):
            for j in range(rings) if d < 3 else ring_half[way]:
                n = d * rings + j
                gather[way, d, j] = copy_to(
                    xm.at[slot(way, d), :, ring_cols(j)], xm.at[slot(way, d + 1), :, ring_cols(j)],
                    ag_s.at[way, n], ag_r.at[way, n], ring[way],
                )
    for k in range(8):
        for n, (begin, end) in enumerate(parts):
            at = pl.ds(begin, end - begin)
            share[k, n] = copy_to(xm.at[k, :, at], xp.at[k, :, at], xs.at[k, n], xrs.at[k, n], partner)

    def trade(g, j):
        at = pl.ds(pl.multiple_of(j * cw, cw), cw)
        pair = pl.ds(2 * g - 2, 2)
        return copy_to(yps.at[pair, :, at], ypr.at[pair, :, at], yss.at[g - 1, j], yrs.at[g - 1, j], partner)

    def hidden_units(g, first, last):
        def piece(k, carry):
            at = pl.ds(pl.multiple_of(k * 256, 256), 256)
            left = xm[2 * g - 2 : 2 * g].reshape(2 * ROWS, half)
            right = xp[2 * g - 2 : 2 * g].reshape(2 * ROWS, half)
            gate = dot(left, wg[0, :, at]) + dot(right, wg[1, :, at])
            lift = dot(left, wu[0, :, at]) + dot(right, wu[1, :, at])
            inner[pl.ds((2 * g - 2) * ROWS, 2 * ROWS), at] = (gate / (1.0 + jnp.exp(-gate)) * lift).astype(BF)
            return carry

        lax.fori_loop(first, last, piece, 0)

    def units_part(g, n, fresh, done):
        begin, end = parts[n]
        at_k = pl.ds(begin, end - begin)

        def piece(k, carry):
            at = pl.ds(pl.multiple_of(k * 256, 256), 256)
            left = xm[2 * g - 2 : 2 * g, :, at_k].reshape(2 * ROWS, end - begin)
            right = xp[2 * g - 2 : 2 * g, :, at_k].reshape(2 * ROWS, end - begin)
            gate = dot(left, wg[0, at_k, at]) + dot(right, wg[1, at_k, at])
            lift = dot(left, wu[0, at_k, at]) + dot(right, wu[1, at_k, at])
            if not fresh:
                gate, lift = gate + partial[0, :, at], lift + partial[1, :, at]
            if done:
                inner[pl.ds((2 * g - 2) * ROWS, 2 * ROWS), at] = (gate / (1.0 + jnp.exp(-gate)) * lift).astype(BF)
            else:
                partial[0, :, at], partial[1, :, at] = gate, lift
            return carry

        lax.fori_loop(0, 2, piece, 0)

    def down_out(g):
        rows = inner[pl.ds((2 * g - 2) * ROWS, 2 * ROWS), :]

        def theirs(j, carry):
            at = pl.ds(pl.multiple_of(j * cw, cw), cw)
            yps[pl.ds(2 * g - 2, 2), :, at] = dot(rows, wd[1, :, at]).astype(BF).reshape(2, ROWS, cw)
            trade(g, j).start()
            return carry

        lax.fori_loop(0, CHUNKS, theirs, 0)

    def down_own(g):
        rows = inner[pl.ds((2 * g - 2) * ROWS, 2 * ROWS), :]

        def mine(j, carry):
            trade(g, j).wait_recv()
            at = pl.ds(pl.multiple_of(j * cw, cw), cw)
            both = dot(rows, wd[0, :, at]).reshape(2, ROWS, cw) + ypr[pl.ds(2 * g - 2, 2), :, at].astype(F32)
            ys[pl.ds(2 * g - 2, 2), :, at] = both.astype(BF)
            return carry

        lax.fori_loop(0, CHUNKS, mine, 0)

    reduce, link = {}, {}
    for way in range(2):
        for d in range(1, 5):
            target = slot(1 - way, d)
            for j in range(rings) if d < 4 else ring_half[way]:
                n = (d - 1) * rings + j
                reduce[way, d, j] = copy_to(
                    ys.at[target, :, ring_cols(j)], rr.at[way, d - 1, :, pl.ds(RING * j, RING)],
                    rs_s.at[way, n], rs_r.at[way, n], ring[way],
                )
            for j in range(2) if d < 4 else (way,):
                at = pl.ds(wide // 2 * j, wide // 2)
                link[way, d, j] = copy_to(
                    cz.at[target, :, at], rc.at[way, d - 1, :, at],
                    cr_s.at[way, 2 * (d - 1) + j], cr_r.at[way, 2 * (d - 1) + j], ring[way],
                )

    def pass_on(way, d, j, add):
        if add:
            reduce[way, d + 1, j].wait_recv()
            k = slot(1 - way, d)
            total = ys[k, :, ring_cols(j)].astype(F32) + rr[way, d, :, pl.ds(RING * j, RING)].astype(F32)
            ys[k, :, ring_cols(j)] = total.astype(BF)
        reduce[way, d, j].start()

    def both_ways(d, lists, add):
        for n in range(max(len(lists[0]), len(lists[1]))):
            for way in range(2):
                if n < len(lists[way]):
                    pass_on(way, d, lists[way][n], add)

    def chain(d):
        for j in range(2):
            at = pl.ds(wide // 2 * j, wide // 2)
            for way in range(2):
                if (way, d, j) in link:
                    if (way, d + 1, j) in link:
                        link[way, d + 1, j].wait_recv()
                        k = slot(1 - way, d)
                        cz[k, :, at] = (cz[k, :, at].astype(F32) + rc[way, d, :, at].astype(F32)).astype(BF)
                    link[way, d, j].start()

    def weigh(k, rows, extra):
        return (
            dot_rows(high[k], rows) + dot_rows(low[k], rows) + dot_rows(ohigh[k], extra) + dot_rows(olow[k], extra)
        )

    def send_back(w):
        start, count = groups[w]
        many, slots, at = pl.ds(0, count), pl.ds(start, count), pl.ds(0, wide)
        for p in range(count):
            tail = ys[start + p, MAIN:, at].astype(F32)
            for q in range(wide // 128):
                pvb[w, :, p, q, :] = tail[:, 128 * q : 128 * (q + 1)]

        @pl.when(own)
        def _():
            rb[w, e * 2 + s, many] = ys[slots, source_rows(e, c), at]
            ovb[w, e, many] = pvb[w, e, many]

        for i in range(8):
            ed = (e + i) % 8
            for k in (1, 0):
                cd = (c + k) % 2
                send(
                    copy_to(
                        ys.at[slots, source_rows(ed, cd), at], rb.at[w, e * 2 + s, many],
                        bw_s.at[w, i * 2 + k], bw_r.at[w, e * 2 + s], (c, ed, z * 2 + cd),
                    ), i, k == 0,
                )
            send(
                copy_to(pvb.at[w, ed, many], ovb.at[w, e, many], vw_s.at[w, i], vw_r.at[w, e], (c, ed, z * 2 + s)),
                i, True,
            )

    def receive_back(w):
        start, count = groups[w]
        many, slots, at = pl.ds(0, count), pl.ds(start, count), pl.ds(0, wide)
        for i in range(8):
            ef = (e + 8 - i) % 8
            for k in range(2):
                sf = (s + k) % 2
                receive(
                    copy_to(
                        ys.at[slots, source_rows(0, 0), at], rb.at[w, ef * 2 + sf, many],
                        bw_s.at[w, 0], bw_r.at[w, ef * 2 + sf], (sf, ef, z * 2 + s),
                    ), i, k == 0,
                )
            receive(
                copy_to(pvb.at[w, 0, many], ovb.at[w, ef, many], vw_s.at[w, 0], vw_r.at[w, ef], (c, ef, z * 2 + s)),
                i, True,
            )
        totals = []
        for p in range(count):
            extra = jnp.concatenate([ovb[w, :, p, q, :] for q in range(wide // 128)], axis=1).astype(BF)
            totals.append(weigh(start + p, rb[w, :, p].reshape(MAIN, wide), extra))
            if w > 0:
                cz[start + p] = totals[p].astype(BF)
        return totals[0]

    send_wide(0)
    carry(1)
    send_wide(1)
    for a in range(3):
        from_col = max(wide, hw * (a + 1))
        width = hw * (a + 2) - from_col
        land = pl.ds(from_col, width)
        part = pl.ds(from_col - wide, width)
        for i in range(8):
            ef = (e + 8 - i) % 8
            for k in range(2):
                cf = (c + k) % 2
                receive(
                    copy_to(
                        pk.at[0, :, part], xm.at[7, source_rows(ef, cf), land],
                        d_s.at[a, 0], d_r.at[a, ef * 2 + cf], (c, ef, z * 2 + cf),
                    ), i, k == 0,
                )
            receive(copy_to(pov.at[a, 0], ovr.at[a, ef], o_s.at[a, 0], o_r.at[a, ef], (c, ef, z * 2 + s)), i, True)
        for q in range(width // 128):
            at = from_col + 128 * q
            xm[7, MAIN:, at : at + 128] = ovr[a, :, q, :].astype(BF)
        for j in range((from_col - wide) // RING, (from_col - wide + width) // RING):
            for way in range(2):
                gather[way, 0, j].start()
        if a == 1:
            carry(2)
    share[7, 1].start()
    share[7, 2].start()
    send_wide(2)
    carry(3)
    send_wide(3)
    for load in loads:
        load.wait()

    receive_wide(0)

    def shared(k):
        for n in range(3):
            share[k, n].wait_recv()

    for d in range(1, 4):
        if d > 1:
            receive_wide(d - 1)
            for way in range(2):
                shared(slot(way, d - 1))
        for j in range(rings):
            for way in range(2):
                gather[way, d - 1, j].wait_recv()
                if (way, d, j) in gather:
                    gather[way, d, j].start()
                if j in (2, rings - 1):
                    share[slot(way, d), 1 + j // 3].start()
            if d == 1 and j == 1:
                carry(4)
                send_wide(4)
            if d > 1 and j in (1, 3):
                hidden_units(d - 1, j // 2, j // 2 + 1)
            if d == 3 and j == 2:
                receive_wide(3)
            if d == 3 and j == 3:
                for way in range(2):
                    share[slot(way, 3), 1].wait_recv()
                units_part(3, 1, True, False)
    receive_wide(4)
    for way in range(2):
        share[slot(way, 3), 2].wait_recv()
    units_part(3, 2, False, False)
    for way in range(2):
        share[slot(way, 3), 0].wait_recv()
    units_part(3, 0, False, True)
    down_out(3)
    down_out(2)
    for way in range(2):
        for j in ring_half[way]:
            gather[way, 3, j].wait_recv()
    share[6, 1].start()
    share[6, 2].start()
    down_own(3)

    swapped = (ring_half[1], ring_half[0])
    orders = tuple(b + a for a, b in zip(ring_half, swapped))
    lasts = (orders[0], (0, 3, 4, 1, 2))
    both_ways(3, swapped, False)
    send_back(3)
    down_own(2)
    shared(6)
    shared(7)
    hidden_units(4, 0, 1)
    both_ways(2, swapped, True)
    hidden_units(4, 1, 2)
    down_out(4)
    down_own(4)
    both_ways(4, ring_half, False)
    send_back(4)
    send_back(2)
    down_out(1)
    receive_back(3)
    both_ways(3, ring_half, True)
    receive_back(4)
    chain(4)
    down_own(1)
    send_back(1)
    send_back(0)
    both_ways(2, ring_half, True)
    chain(3)
    receive_back(2)
    both_ways(1, tuple(o[:2] for o in lasts), True)
    chain(2)
    receive_back(1)
    both_ways(1, tuple(o[2:4] for o in lasts), True)
    chain(1)
    both_ways(1, tuple(o[4:] for o in lasts), True)

    pieces = ((3, 2), (0, 2), (2, 1))
    for a, (j, count) in enumerate(pieces):
        width = count * RING
        for n in range(j, j + count):
            for way in range(2):
                reduce[way, 1, n].wait_recv()
        land, part = pl.ds(wide + RING * j, width), pl.ds(RING * j, width)
        total = (
            ys[7, :, land].astype(F32) + rr[0, 0, :, part].astype(F32) + rr[1, 0, :, part].astype(F32)
        ).astype(BF)
        ys[7, :, land] = total
        tail = total[MAIN:].astype(F32)
        for q in range(width // 128):
            fov[a, :, q, :] = tail[:, 128 * q : 128 * (q + 1)]

        @pl.when(own)
        def _():
            ret[e * 2 + s, :, part] = ys[7, source_rows(e, c), land]
            retov[a, e] = fov[a, e]

        for i in range(8):
            ed = (e + i) % 8
            for k in (1, 0):
                cd = (c + k) % 2
                send(
                    copy_to(
                        ys.at[7, source_rows(ed, cd), land], ret.at[e * 2 + s, :, part],
                        b_s.at[a, i * 2 + k], b_r.at[a, e * 2 + s], (c, ed, z * 2 + cd),
                    ), i, k == 0,
                )
            send(copy_to(fov.at[a, ed], retov.at[a, e], bo_s.at[a, i], bo_r.at[a, e], (c, ed, z * 2 + s)), i, True)

    total = receive_back(0)
    for way in range(2):
        for j in range(2):
            link[way, 1, j].wait_recv()
        total = total + rc[way, 0].astype(F32)
    out[0, :, 0:wide] = (hid[:, 0:wide].astype(F32) + total).astype(BF)

    for a, (j, count) in enumerate(pieces):
        width = count * RING
        land, part = pl.ds(wide + RING * j, width), pl.ds(RING * j, width)
        for i in range(8):
            ef = (e + 8 - i) % 8
            for k in range(2):
                sf = (s + k) % 2
                receive(
                    copy_to(
                        ys.at[7, source_rows(0, 0), land], ret.at[ef * 2 + sf, :, part],
                        b_s.at[a, 0], b_r.at[a, ef * 2 + sf], (sf, ef, z * 2 + s),
                    ), i, k == 0,
                )
            receive(copy_to(fov.at[a, 0], retov.at[a, ef], bo_s.at[a, 0], bo_r.at[a, ef], (c, ef, z * 2 + s)), i, True)
        extra = jnp.concatenate([retov[a, :, q, :] for q in range(width // 128)], axis=1).astype(BF)
        total = weigh(7, ret[:, :, part].reshape(MAIN, width), extra)
        out[0, :, land] = (hid[:, land].astype(F32) + total).astype(BF)

    @pl.when(jnp.logical_not(own))
    def _():
        for copy in own_sent:
            copy.wait_send()
    for copy in sent:
        copy.wait_send()
    for way in range(2):
        for d in range(4):
            for h in range(kv_heads) if d < 3 else half_of[way]:
                spread(way, d, h).wait_send()
    for k in range(8):
        for h in range(kv_heads):
            swap(k, h).wait_send()
    for copy in tell:
        copy.wait_send()
    for g in range(1, 5):
        for j in range(CHUNKS):
            trade(g, j).wait_send()
    for table in (carry_on, gather, share, reduce, link):
        for copy in table.values():
            copy.wait_send()


def on_device(query, keys, values, residual, routes, gates, w_gate, w_up, w_down):
    _, tokens, half = query.shape
    units = w_gate.shape[2]
    kv_heads = keys.shape[2] // HD
    stacked = half // HD // kv_heads * tokens
    vmem = pl.BlockSpec(memory_space=pltpu.VMEM)
    hbm = pl.BlockSpec(memory_space=pl.ANY)
    dma = pltpu.SemaphoreType.DMA
    return pl.pallas_call(
        layer_kernel,
        out_shape=jax.ShapeDtypeStruct(query.shape, BF),
        in_specs=[hbm] * 4 + [vmem] * 2 + [hbm] * 3,
        out_specs=vmem,
        scratch_shapes=[
            pltpu.VMEM((tokens, half), BF),
            pltpu.VMEM((tokens, half), BF),
            pltpu.VMEM((8, 2, kv_heads, 2, tokens, HD), BF),
            pltpu.VMEM((kv_heads, stacked, HD), BF),
            pltpu.VMEM((kv_heads, stacked, 1), F32),
            pltpu.VMEM((kv_heads, stacked, HD), F32),
            pltpu.VMEM((kv_heads, stacked, HD), F32),
            pltpu.VMEM((tokens, half), BF),
            pltpu.VMEM((8, 8, 128), F32),
            pltpu.VMEM((8, MAIN, tokens), BF),
            pltpu.VMEM((8, EXPERTS, tokens), BF),
            pltpu.VMEM((8, MAIN, tokens), BF),
            pltpu.VMEM((8, MAIN, tokens), BF),
            pltpu.VMEM((8, EXPERTS, tokens), BF),
            pltpu.VMEM((8, EXPERTS, tokens), BF),
            pltpu.VMEM((8, tokens, WIDE), BF),
            pltpu.VMEM((2, half, units), BF),
            pltpu.VMEM((2, half, units), BF),
            pltpu.VMEM((2, units, half), BF),
            pltpu.VMEM((16, SLOTS, half - WIDE), BF),
            pltpu.VMEM((3, 8, 8, 128), F32),
            pltpu.VMEM((3, 8, 8, 128), F32),
            pltpu.VMEM((5, 16, 2, SLOTS, WIDE), BF),
            pltpu.VMEM((5, 8, 2, 8, 128), F32),
            pltpu.VMEM((5, 8, 2, 8, 128), F32),
            pltpu.VMEM((8, ROWS, half), BF),
            pltpu.VMEM((8, ROWS, half), BF),
            pltpu.VMEM((2, 2 * ROWS, units), F32),
            pltpu.VMEM((8 * ROWS, units), BF),
            pltpu.VMEM((8, ROWS, half), BF),
            pltpu.VMEM((8, ROWS, half), BF),
            pltpu.VMEM((8, ROWS, half), BF),
            pltpu.VMEM((2, 4, ROWS, half - WIDE), BF),
            pltpu.VMEM((3, 8, 8, 128), F32),
            pltpu.VMEM((16, SLOTS, half - WIDE), BF),
            pltpu.VMEM((3, 8, 8, 128), F32),
            pltpu.VMEM((5, 16, 2, SLOTS, WIDE), BF),
            pltpu.VMEM((5, 8, 2, 8, 128), F32),
            pltpu.VMEM((5, 8, 2, 8, 128), F32),
            pltpu.VMEM((8, tokens, WIDE), BF),
            pltpu.VMEM((2, 4, tokens, WIDE), BF),
            dma((10,)), dma((7,)), dma((7,)), dma((2, 16)), dma((2, 16)), dma((8, 4)), dma((8, 4)),
            dma((2, 8)), dma((2, 8)), dma((5, 16)), dma((5, 16)), dma((5, 8)), dma((5, 8)),
            dma((6,)), dma((3, 16)), dma((3, 16)), dma((3, 8)), dma((3, 8)),
            dma((2, 32)), dma((2, 32)), dma((8, 3)), dma((8, 3)), dma((4, 4)), dma((4, 4)),
            dma((2, 32)), dma((2, 32)), dma((3, 16)), dma((3, 16)), dma((3, 8)), dma((3, 8)),
            dma((5, 16)), dma((5, 16)), dma((5, 8)), dma((5, 8)), dma((2, 8)), dma((2, 8)),
        ],
        compiler_params=pltpu.CompilerParams(
            collective_id=1, has_side_effects=True, vmem_limit_bytes=60 * 1024 * 1024
        ),
        name="layer",
    )(query, keys, values, residual, routes[0].T, gates[0].T, w_gate, w_up, w_down)


def solution(mesh):
    return jax.shard_map(
        on_device,
        mesh=mesh,
        in_specs=(
            P("expert", "tensor", "section"),
            P("expert", "tensor", "section"),
            P("expert", "tensor", "section"),
            P("expert", "tensor", "section"),
            P("expert", "tensor", None),
            P("expert", "tensor", None),
            P("expert", None, "tensor"),
            P("expert", None, "tensor"),
            P("expert", "tensor", None),
        ),
        out_specs=P("expert", "tensor", "section"),
        check_vma=False,
    )
```

```python
import math

import jax
import jax.numpy as jnp
from jax import lax
from jax.experimental import pallas as pl
from jax.experimental.pallas import tpu as pltpu
from jax.sharding import PartitionSpec as P

HD = 128
EXPERTS = 8
NZ = 8
SLOTS = 8
MAIN = 2 * SLOTS * EXPERTS
ROWS = MAIN + EXPERTS
CHUNKS = 4
WIDE = 768
RING = 256
FAR = (0, 2, 4, 6, 5, 3, 1)
MESH = pl.DeviceIdType.MESH
BF = jnp.bfloat16
F32 = jnp.float32


def dot(a, b):
    return jnp.dot(a, b, preferred_element_type=F32)


def landed(ref, sem):
    pltpu.make_async_copy(ref, ref, sem).wait()


def dot_rows(a, b):
    return lax.dot_general(a, b, (((0,), (0,)), ((), ())), preferred_element_type=F32)


def copy_to(src, dst, send, recv, device):
    return pltpu.make_async_remote_copy(
        src_ref=src, dst_ref=dst, send_sem=send, recv_sem=recv, device_id=device, device_id_type=MESH
    )


def layer_kernel(
    q_any, k_any, v_any, res_any, routes, gates, wg_any, wu_any, wd_any, out,
    qv, res, kv, qs, top, mass, acc, hid, rz, hits, overs, high, low, ohigh, olow, hz,
    wg, wu, wd, pk, pov, ovr, pw, pvw, ovw, xm, xp, partial, inner, yps, ypr, ys, rr, fov, ret, retov,
    rb, pvb, ovb, cz, rc,
    in_sem, rz_s, rz_r, kg_s, kg_r, kx_s, kx_r, hz_s, hz_r, dw_s, dw_r, ow_s, ow_r,
    w_sem, d_s, d_r, o_s, o_r, ag_s, ag_r, xs, xrs, yss, yrs, rs_s, rs_r, b_s, b_r, bo_s, bo_r,
    bw_s, bw_r, vw_s, vw_r, cr_s, cr_r,
):
    s, e, t = lax.axis_index("section"), lax.axis_index("expert"), lax.axis_index("tensor")
    z, c = t // 2, t % 2
    tokens, half = hid.shape
    cw = half // CHUNKS
    kv_heads = qs.shape[0]
    own_in = []
    for h in range(kv_heads):
        at = pl.ds(HD * h, HD)
        own_in.append(pltpu.make_async_copy(k_any.at[0, :, at], kv.at[7, 0, h, 0], in_sem.at[0]))
        own_in.append(pltpu.make_async_copy(v_any.at[0, :, at], kv.at[7, 0, h, 1], in_sem.at[0]))
    queries_in = pltpu.make_async_copy(q_any.at[0], qv, in_sem.at[1])
    residual_in = pltpu.make_async_copy(res_any.at[0], res, in_sem.at[2])
    own_in += [queries_in, residual_in]
    for load in own_in:
        load.start()
    barrier = pltpu.get_barrier_semaphore()
    for i in range(1, 32):
        other = (s * 2 + c) ^ (i % 4)
        pl.semaphore_signal(
            barrier, inc=1, device_id=(other // 2, (e + i // 4) % 8, z * 2 + other % 2), device_id_type=MESH
        )
    up, down = (z + 1) % NZ, (z + NZ - 1) % NZ
    for k in range(1, NZ):
        pl.semaphore_signal(barrier, inc=1, device_id=(s, e, ((z + k) % NZ) * 2 + c), device_id_type=MESH)
    rz[7] = jnp.zeros(rz.shape[1:], F32)
    rz[7, 0:2, 0:tokens] = routes[...].astype(F32)
    rz[7, 2:4, 0:tokens] = gates[...]
    loads = []
    for part in range(2):
        h = (c + part) % 2
        rows = pl.ds(pl.multiple_of(h * half, half), half)
        loads.append(pltpu.make_async_copy(wg_any.at[0, rows, :], wg.at[part], w_sem.at[part]))
        loads.append(pltpu.make_async_copy(wu_any.at[0, rows, :], wu.at[part], w_sem.at[2 + part]))
        loads.append(pltpu.make_async_copy(wd_any.at[0, :, rows], wd.at[part], w_sem.at[4 + part]))

    def slot(way, d):
        return 7 if d == 0 else 6 if d == 4 else 2 * (d - 1) + way

    partner = (s, e, z * 2 + 1 - c)
    ring = ((s, e, up * 2 + c), (s, e, down * 2 + c))

    def spread(way, d, h):
        return copy_to(
            kv.at[slot(way, d), 0, h], kv.at[slot(way, d + 1), 0, h],
            kg_s.at[way, d // 3], kg_r.at[way, 4 * d + h], ring[way],
        )

    def swap(k, h):
        return copy_to(kv.at[k, 0, h], kv.at[k, 1, h], kx_s.at[0], kx_r.at[k, h], partner)

    tell = [
        copy_to(rz.at[7], rz.at[FAR[k - 1]], rz_s.at[0], rz_r.at[0], (s, e, ((z + k) % NZ) * 2 + c))
        for k in range(1, NZ)
    ]
    landed(kv.at[7, 0], in_sem.at[0])
    pl.semaphore_wait(barrier, 38)
    for h in range(kv_heads):
        for way in range(2):
            spread(way, 0, h).start()
        swap(7, h).start()
    for copy in tell:
        copy.start()
    for load in loads:
        load.start()

    earlier = (
        lax.broadcasted_iota(jnp.int32, (tokens, tokens), 0) < lax.broadcasted_iota(jnp.int32, (tokens, tokens), 1)
    ).astype(BF)

    line = lax.broadcasted_iota(jnp.int32, (MAIN, tokens), 0)
    few = lax.broadcasted_iota(jnp.int32, (EXPERTS, tokens), 0)

    def placed(k, expert, wanted, hit_ref, high_ref, low_ref):
        is0, is1 = (rz[k, n : n + 1, 0:tokens] == expert.astype(F32) for n in range(2))
        gate0, gate1 = (rz[k, n : n + 1, 0:tokens] for n in (2, 3))
        named = jnp.where(is0 | is1, 1.0, 0.0)
        place = dot(named.astype(BF), earlier)
        hit = jnp.where(place == wanted.astype(F32), named, 0.0)
        weight = hit * (jnp.where(is0, gate0, 0.0) + jnp.where(is1, gate1, 0.0))
        top_part = weight.astype(BF)
        hit_ref[k] = hit.astype(BF)
        high_ref[k] = top_part
        low_ref[k] = (weight - top_part.astype(F32)).astype(BF)

    def slot_tables(k):
        placed(k, line // (2 * SLOTS), line % (2 * SLOTS), hits, high, low)
        placed(k, few, jnp.full_like(few, 2 * SLOTS), overs, ohigh, olow)

    slot_tables(7)
    queries_in.wait()
    group = qs.shape[1] // tokens
    for h in range(kv_heads):
        for g in range(group):
            qs[h, tokens * g : tokens * (g + 1), :] = qv[:, HD * (h * group + g) : HD * (h * group + g + 1)]
    stacked = group * tokens
    scale = math.log2(math.e) / math.sqrt(HD)

    def attend(start, count, bias, fresh, h):
        keys = count * 2 * tokens
        k = kv[start : start + count, :, h, 0].reshape(keys, HD)
        v = kv[start : start + count, :, h, 1].reshape(keys, HD)
        scores = lax.dot_general(qs[h], k, (((1,), (1,)), ((), ())), preferred_element_type=F32) * scale + bias
        peak = jnp.max(scores, axis=1, keepdims=True)
        if not fresh:
            peak = jnp.maximum(peak, top[h])
        terms = jnp.exp2(scores - peak).astype(BF)
        both = dot(terms, jnp.concatenate([v, jnp.ones_like(v)], axis=1))
        context, total = both[:, :HD], both[:, HD:]
        if not fresh:
            fade = jnp.exp2(top[h] - peak)
            total = total + mass[h] * fade
            context = context + acc[h] * fade
        top[h], mass[h], acc[h] = peak, total, context

    row = lax.broadcasted_iota(jnp.int32, (stacked, 2 * tokens), 0) % tokens
    col = lax.broadcasted_iota(jnp.int32, (stacked, 2 * tokens), 1)
    diagonal = jnp.where(col <= jnp.where(col < tokens, row, jnp.where(c == 1, 2 * tokens, -1)), 0.0, -1e30)

    def ring_bias(d):
        col = lax.broadcasted_iota(jnp.int32, (1, (2 if d < 4 else 1) * 2 * tokens), 1)
        return jnp.where(jnp.where(col < 2 * tokens, z - d, z + d - NZ) >= 0, 0.0, -1e30)

    def first_step(h, carry):
        swap(7, h).wait_recv()
        attend(7, 1, diagonal, True, h)
        return carry

    lax.fori_loop(0, kv_heads, first_step, 0)
    for d in range(1, 4):
        bias = ring_bias(d - 1) if d > 1 else None

        def ring_step(h, carry, d=d, bias=bias):
            for way in range(2):
                spread(way, d - 1, h).wait_recv()
                if d < 3:
                    spread(way, d, h).start()
                else:
                    pl.when(h // 2 == way)(spread(way, d, h).start)
                swap(slot(way, d), h).start()
            if d > 1:
                for way in range(2):
                    swap(slot(way, d - 1), h).wait_recv()
                attend(slot(0, d - 1), 2, bias, False, h)
            return carry

        lax.fori_loop(0, kv_heads, ring_step, 0)
    bias = ring_bias(3)

    def last_step(h, carry):
        for way in range(2):
            swap(slot(way, 3), h).wait_recv()
        attend(slot(0, 3), 2, bias, False, h)
        return carry

    bias4 = ring_bias(4)
    landed(rz.at[pl.ds(0, 7)], rz_r.at[0])
    for k in range(7):
        slot_tables(k)
    for h in range(2):
        last_step(h, 0)
        for way in range(2):
            spread(way, 3, 2 * way + h).wait_recv()
            swap(6, 2 * way + h).start()
    residual_in.wait()

    own = s == c
    wide = WIDE
    rings = (half - wide) // RING
    ring_half = (tuple(range((rings + 1) // 2)), tuple(range((rings + 1) // 2, rings)))
    hw = half // kv_heads

    def ring_cols(j):
        return pl.ds(wide + RING * j, RING)

    def send(copy, i, same):
        if i == 0 and same:
            pl.when(jnp.logical_not(own))(copy.start)
        else:
            copy.start()

    def settle(ref, sem, axis):
        index = [slice(None)] * len(ref.shape)
        index[axis] = pl.ds(0, ref.shape[axis] - ref.shape[axis] // (16 if ref.shape[axis] > 8 else 8))
        fewer = tuple(pl.ds(0, n) if isinstance(i, slice) else i for i, n in zip(index, ref.shape))

        @pl.when(own)
        def _():
            landed(ref.at[fewer], sem)

        @pl.when(jnp.logical_not(own))
        def _():
            landed(ref, sem)

    def source_rows(ef, cf):
        return pl.ds(pl.multiple_of((ef * 2 + cf) * SLOTS, SLOTS), SLOTS)

    carry_on = {}
    for way in range(2):
        for d in range(4):
            for j in range(2) if d < 3 else (way,):
                at = pl.ds(wide // 2 * j, wide // 2)
                carry_on[way, d, j] = copy_to(
                    hz.at[slot(way, d), :, at], hz.at[slot(way, d + 1), :, at],
                    hz_s.at[way, d // 3], hz_r.at[way, 2 * d + j], ring[way],
                )

    for h in range(kv_heads):
        swap(6, h).wait_recv()
        if h >= 2:
            last_step(h, 0)
        attend(6, 1, bias4, False, h)
        context = acc[h] / mass[h]
        for g in range(group):
            at = slice(HD * (h * group + g), HD * (h * group + g + 1))
            hid[:, at] = (res[:, at].astype(F32) + context[tokens * g : tokens * (g + 1), :]).astype(BF)
        from_col = hw * h
        if from_col < wide:
            to_col = min(wide, from_col + hw)
            hz[7, :, from_col:to_col] = hid[:, from_col:to_col]
            for j in range(2):
                if from_col < wide // 2 * (j + 1) <= to_col:
                    for way in range(2):
                        carry_on[way, 0, j].start()
        if h == 0:
            continue
        a = h - 1
        from_col = max(from_col, wide)
        width = hw * (h + 1) - from_col
        piece = hid[:, from_col : from_col + width]
        part = pl.ds(from_col - wide, width)
        pk[:, :, part] = dot(hits[7], piece).astype(BF).reshape(16, SLOTS, width)
        extra = dot(overs[7], piece)
        for q in range(width // 128):
            pov[a, :, q, :] = extra[:, 128 * q : 128 * (q + 1)]
        land = pl.ds(from_col, width)

        @pl.when(own)
        def _():
            xm[7, source_rows(e, c), land] = pk[e * 2 + s, :, part]
            ovr[a, e] = pov[a, e]

        for i in range(8):
            ed = (e + i) % 8
            for k in (1, 0):
                sd = (s + k) % 2
                send(
                    copy_to(
                        pk.at[ed * 2 + sd, :, part], xm.at[7, source_rows(e, c), land],
                        d_s.at[a], d_r.at[a], (sd, ed, z * 2 + s),
                    ), i, k == 0,
                )
            send(copy_to(pov.at[a, ed], ovr.at[a, e], o_s.at[a], o_r.at[a], (c, ed, z * 2 + s)), i, True)

    groups = ((7, 1), (0, 2), (2, 2), (4, 2), (6, 1))

    def send_wide(w):
        start, count = groups[w]
        for p in range(count):
            tokens_of = hz[start + p]
            pw[w, :, p] = dot(hits[start + p], tokens_of).astype(BF).reshape(16, SLOTS, wide)
            extra = dot(overs[start + p], tokens_of)
            for q in range(wide // 128):
                pvw[w, :, p, q, :] = extra[:, 128 * q : 128 * (q + 1)]
        many = pl.ds(0, count)
        slots = pl.ds(start, count)
        at = pl.ds(0, wide)

        @pl.when(own)
        def _():
            xm[slots, source_rows(e, c), at] = pw[w, e * 2 + s, many]
            ovw[w, e, many] = pvw[w, e, many]

        for i in range(8):
            ed = (e + i) % 8
            for k in (1, 0):
                sd = (s + k) % 2
                send(
                    copy_to(
                        pw.at[w, ed * 2 + sd, many], xm.at[slots, source_rows(e, c), at],
                        dw_s.at[w], dw_r.at[w], (sd, ed, z * 2 + s),
                    ), i, k == 0,
                )
            send(
                copy_to(pvw.at[w, ed, many], ovw.at[w, e, many], ow_s.at[w], ow_r.at[w], (c, ed, z * 2 + s)),
                i, True,
            )

    def receive_wide(w):
        start, count = groups[w]
        many = pl.ds(0, count)
        slots = pl.ds(start, count)
        at = pl.ds(0, wide)
        settle(xm.at[slots, pl.ds(0, MAIN), at], dw_r.at[w], 1)
        settle(ovw.at[w, :, many], ow_r.at[w], 0)
        for p in range(count):
            for q in range(wide // 128):
                xm[start + p, MAIN:, 128 * q : 128 * (q + 1)] = ovw[w, :, p, q, :].astype(BF)
            share[start + p, 0].start()

    def carry(d):
        for j in range(2):
            for way in range(2) if d < 4 else (j,):
                carry_on[way, d - 1, j].wait_recv()
                if (way, d, j) in carry_on:
                    carry_on[way, d, j].start()

    def cols(j):
        return pl.ds(cw * j, cw)

    half_of = ((0, 1), (2, 3))
    gather, share = {}, {}
    split = wide + 3 * RING
    parts = ((0, wide), (wide, split), (split, half))
    for way in range(2):
        for d in range(4):
            for j in range(rings) if d < 3 else ring_half[way]:
                n = d * rings + j
                gather[way, d, j] = copy_to(
                    xm.at[slot(way, d), :, ring_cols(j)], xm.at[slot(way, d + 1), :, ring_cols(j)],
                    ag_s.at[way, d // 3], ag_r.at[way, n], ring[way],
                )
    for k in range(8):
        for n, (begin, end) in enumerate(parts):
            at = pl.ds(begin, end - begin)
            share[k, n] = copy_to(xm.at[k, :, at], xp.at[k, :, at], xs.at[0], xrs.at[k, n], partner)

    def trade(g, j):
        at = pl.ds(pl.multiple_of(j * cw, cw), cw)
        pair = pl.ds(2 * g - 2, 2)
        return copy_to(yps.at[pair, :, at], ypr.at[pair, :, at], yss.at[0], yrs.at[g - 1, j], partner)

    def hidden_units(g, first, last):
        def piece(k, carry):
            at = pl.ds(pl.multiple_of(k * 256, 256), 256)
            left = xm[2 * g - 2 : 2 * g].reshape(2 * ROWS, half)
            right = xp[2 * g - 2 : 2 * g].reshape(2 * ROWS, half)
            gate = dot(left, wg[0, :, at]) + dot(right, wg[1, :, at])
            lift = dot(left, wu[0, :, at]) + dot(right, wu[1, :, at])
            inner[pl.ds((2 * g - 2) * ROWS, 2 * ROWS), at] = (gate / (1.0 + jnp.exp(-gate)) * lift).astype(BF)
            return carry

        lax.fori_loop(first, last, piece, 0)

    def units_part(g, n, fresh, done):
        begin, end = parts[n]
        at_k = pl.ds(begin, end - begin)

        def piece(k, carry):
            at = pl.ds(pl.multiple_of(k * 256, 256), 256)
            left = xm[2 * g - 2 : 2 * g, :, at_k].reshape(2 * ROWS, end - begin)
            right = xp[2 * g - 2 : 2 * g, :, at_k].reshape(2 * ROWS, end - begin)
            gate = dot(left, wg[0, at_k, at]) + dot(right, wg[1, at_k, at])
            lift = dot(left, wu[0, at_k, at]) + dot(right, wu[1, at_k, at])
            if not fresh:
                gate, lift = gate + partial[0, :, at], lift + partial[1, :, at]
            if done:
                inner[pl.ds((2 * g - 2) * ROWS, 2 * ROWS), at] = (gate / (1.0 + jnp.exp(-gate)) * lift).astype(BF)
            else:
                partial[0, :, at], partial[1, :, at] = gate, lift
            return carry

        lax.fori_loop(0, 2, piece, 0)

    def down_out(g):
        rows = inner[pl.ds((2 * g - 2) * ROWS, 2 * ROWS), :]

        def theirs(j, carry):
            at = pl.ds(pl.multiple_of(j * cw, cw), cw)
            yps[pl.ds(2 * g - 2, 2), :, at] = dot(rows, wd[1, :, at]).astype(BF).reshape(2, ROWS, cw)
            trade(g, j).start()
            return carry

        lax.fori_loop(0, CHUNKS, theirs, 0)

    def down_own(g):
        rows = inner[pl.ds((2 * g - 2) * ROWS, 2 * ROWS), :]

        def mine(j, carry):
            trade(g, j).wait_recv()
            at = pl.ds(pl.multiple_of(j * cw, cw), cw)
            both = dot(rows, wd[0, :, at]).reshape(2, ROWS, cw) + ypr[pl.ds(2 * g - 2, 2), :, at].astype(F32)
            ys[pl.ds(2 * g - 2, 2), :, at] = both.astype(BF)
            return carry

        lax.fori_loop(0, CHUNKS, mine, 0)

    reduce, link = {}, {}
    for way in range(2):
        for d in range(1, 5):
            target = slot(1 - way, d)
            for j in range(rings) if d < 4 else ring_half[way]:
                n = (d - 1) * rings + j
                reduce[way, d, j] = copy_to(
                    ys.at[target, :, ring_cols(j)], rr.at[way, d - 1, :, pl.ds(RING * j, RING)],
                    rs_s.at[way, d // 4], rs_r.at[way, n], ring[way],
                )
            for j in range(2) if d < 4 else (way,):
                at = pl.ds(wide // 2 * j, wide // 2)
                link[way, d, j] = copy_to(
                    cz.at[target, :, at], rc.at[way, d - 1, :, at],
                    cr_s.at[way, d // 4], cr_r.at[way, 2 * (d - 1) + j], ring[way],
                )

    def pass_on(way, d, j, add):
        if add:
            reduce[way, d + 1, j].wait_recv()
            k = slot(1 - way, d)
            total = ys[k, :, ring_cols(j)].astype(F32) + rr[way, d, :, pl.ds(RING * j, RING)].astype(F32)
            ys[k, :, ring_cols(j)] = total.astype(BF)
        reduce[way, d, j].start()

    def both_ways(d, lists, add):
        for n in range(max(len(lists[0]), len(lists[1]))):
            for way in range(2):
                if n < len(lists[way]):
                    pass_on(way, d, lists[way][n], add)

    def chain(d):
        for j in range(2):
            at = pl.ds(wide // 2 * j, wide // 2)
            for way in range(2):
                if (way, d, j) in link:
                    if (way, d + 1, j) in link:
                        link[way, d + 1, j].wait_recv()
                        k = slot(1 - way, d)
                        cz[k, :, at] = (cz[k, :, at].astype(F32) + rc[way, d, :, at].astype(F32)).astype(BF)
                    link[way, d, j].start()

    def weigh(k, rows, extra):
        return (
            dot_rows(high[k], rows) + dot_rows(low[k], rows) + dot_rows(ohigh[k], extra) + dot_rows(olow[k], extra)
        )

    def send_back(w):
        start, count = groups[w]
        many, slots, at = pl.ds(0, count), pl.ds(start, count), pl.ds(0, wide)
        for p in range(count):
            tail = ys[start + p, MAIN:, at].astype(F32)
            for q in range(wide // 128):
                pvb[w, :, p, q, :] = tail[:, 128 * q : 128 * (q + 1)]

        @pl.when(own)
        def _():
            rb[w, e * 2 + s, many] = ys[slots, source_rows(e, c), at]
            ovb[w, e, many] = pvb[w, e, many]

        for i in range(8):
            ed = (e + i) % 8
            for k in (1, 0):
                cd = (c + k) % 2
                send(
                    copy_to(
                        ys.at[slots, source_rows(ed, cd), at], rb.at[w, e * 2 + s, many],
                        bw_s.at[w], bw_r.at[w], (c, ed, z * 2 + cd),
                    ), i, k == 0,
                )
            send(
                copy_to(pvb.at[w, ed, many], ovb.at[w, e, many], vw_s.at[w], vw_r.at[w], (c, ed, z * 2 + s)),
                i, True,
            )

    def receive_back(w):
        start, count = groups[w]
        many, slots, at = pl.ds(0, count), pl.ds(start, count), pl.ds(0, wide)
        settle(rb.at[w, :, many], bw_r.at[w], 0)
        settle(ovb.at[w, :, many], vw_r.at[w], 0)
        totals = []
        for p in range(count):
            extra = jnp.concatenate([ovb[w, :, p, q, :] for q in range(wide // 128)], axis=1).astype(BF)
            totals.append(weigh(start + p, rb[w, :, p].reshape(MAIN, wide), extra))
            if w > 0:
                cz[start + p] = totals[p].astype(BF)
        return totals[0]

    send_wide(0)
    carry(1)
    send_wide(1)
    for a in range(3):
        from_col = max(wide, hw * (a + 1))
        width = hw * (a + 2) - from_col
        land = pl.ds(from_col, width)
        part = pl.ds(from_col - wide, width)
        settle(xm.at[7, pl.ds(0, MAIN), land], d_r.at[a], 0)
        settle(ovr.at[a], o_r.at[a], 0)
        for q in range(width // 128):
            at = from_col + 128 * q
            xm[7, MAIN:, at : at + 128] = ovr[a, :, q, :].astype(BF)
        for j in range((from_col - wide) // RING, (from_col - wide + width) // RING):
            for way in range(2):
                gather[way, 0, j].start()
        if a == 1:
            carry(2)
    share[7, 1].start()
    share[7, 2].start()
    send_wide(2)
    carry(3)
    send_wide(3)
    for load in loads:
        load.wait()

    receive_wide(0)

    def shared(k):
        for n in range(3):
            share[k, n].wait_recv()

    for d in range(1, 4):
        if d > 1:
            receive_wide(d - 1)
            for way in range(2):
                shared(slot(way, d - 1))
        for j in range(rings):
            for way in range(2):
                gather[way, d - 1, j].wait_recv()
                if (way, d, j) in gather:
                    gather[way, d, j].start()
                if j in (2, rings - 1):
                    share[slot(way, d), 1 + j // 3].start()
            if d == 1 and j == 1:
                carry(4)
                send_wide(4)
            if d > 1 and j in (1, 3):
                hidden_units(d - 1, j // 2, j // 2 + 1)
            if d == 3 and j == 2:
                receive_wide(3)
            if d == 3 and j == 3:
                for way in range(2):
                    share[slot(way, 3), 1].wait_recv()
                units_part(3, 1, True, False)
    receive_wide(4)
    for way in range(2):
        share[slot(way, 3), 2].wait_recv()
    units_part(3, 2, False, False)
    for way in range(2):
        share[slot(way, 3), 0].wait_recv()
    units_part(3, 0, False, True)
    down_out(3)
    down_out(2)
    for way in range(2):
        for j in ring_half[way]:
            gather[way, 3, j].wait_recv()
    share[6, 1].start()
    share[6, 2].start()
    down_own(3)

    swapped = (ring_half[1], ring_half[0])
    orders = tuple(b + a for a, b in zip(ring_half, swapped))
    lasts = (orders[0], (0, 3, 4, 1, 2))
    both_ways(3, swapped, False)
    send_back(3)
    down_own(2)
    shared(6)
    shared(7)
    hidden_units(4, 0, 1)
    both_ways(2, swapped, True)
    hidden_units(4, 1, 2)
    down_out(4)
    down_own(4)
    both_ways(4, ring_half, False)
    send_back(4)
    send_back(2)
    down_out(1)
    receive_back(3)
    both_ways(3, ring_half, True)
    receive_back(4)
    chain(4)
    down_own(1)
    send_back(1)
    send_back(0)
    both_ways(2, ring_half, True)
    chain(3)
    receive_back(2)
    both_ways(1, tuple(o[:2] for o in lasts), True)
    chain(2)
    receive_back(1)
    both_ways(1, tuple(o[2:4] for o in lasts), True)
    chain(1)
    both_ways(1, tuple(o[4:] for o in lasts), True)

    pieces = ((3, 2), (0, 2), (2, 1))
    for a, (j, count) in enumerate(pieces):
        width = count * RING
        for n in range(j, j + count):
            for way in range(2):
                reduce[way, 1, n].wait_recv()
        land, part = pl.ds(wide + RING * j, width), pl.ds(RING * j, width)
        total = (
            ys[7, :, land].astype(F32) + rr[0, 0, :, part].astype(F32) + rr[1, 0, :, part].astype(F32)
        ).astype(BF)
        ys[7, :, land] = total
        tail = total[MAIN:].astype(F32)
        for q in range(width // 128):
            fov[a, :, q, :] = tail[:, 128 * q : 128 * (q + 1)]

        @pl.when(own)
        def _():
            ret[e * 2 + s, :, part] = ys[7, source_rows(e, c), land]
            retov[a, e] = fov[a, e]

        for i in range(8):
            ed = (e + i) % 8
            for k in (1, 0):
                cd = (c + k) % 2
                send(
                    copy_to(
                        ys.at[7, source_rows(ed, cd), land], ret.at[e * 2 + s, :, part],
                        b_s.at[a], b_r.at[a], (c, ed, z * 2 + cd),
                    ), i, k == 0,
                )
            send(copy_to(fov.at[a, ed], retov.at[a, e], bo_s.at[a], bo_r.at[a], (c, ed, z * 2 + s)), i, True)

    total = receive_back(0)
    for way in range(2):
        for j in range(2):
            link[way, 1, j].wait_recv()
        total = total + rc[way, 0].astype(F32)
    out[0, :, 0:wide] = (hid[:, 0:wide].astype(F32) + total).astype(BF)

    for a, (j, count) in enumerate(pieces):
        width = count * RING
        land, part = pl.ds(wide + RING * j, width), pl.ds(RING * j, width)
        settle(ret.at[:, :, part], b_r.at[a], 0)
        settle(retov.at[a], bo_r.at[a], 0)
        extra = jnp.concatenate([retov[a, :, q, :] for q in range(width // 128)], axis=1).astype(BF)
        total = weigh(7, ret[:, :, part].reshape(MAIN, width), extra)
        out[0, :, land] = (hid[:, land].astype(F32) + total).astype(BF)

    for a in range(3):
        from_col = max(wide, hw * (a + 1))
        part = pl.ds(from_col - wide, hw * (a + 2) - from_col)
        settle(pk.at[:, :, part], d_s.at[a], 0)
        settle(pov.at[a], o_s.at[a], 0)
        settle(ret.at[:, :, pl.ds(RING * pieces[a][0], RING * pieces[a][1])], b_s.at[a], 0)
        settle(fov.at[a], bo_s.at[a], 0)
    for w, (start, count) in enumerate(groups):
        many = pl.ds(0, count)
        settle(pw.at[w, :, many], dw_s.at[w], 0)
        settle(pvw.at[w, :, many], ow_s.at[w], 0)
        settle(rb.at[w, :, many], bw_s.at[w], 0)
        settle(pvb.at[w, :, many], vw_s.at[w], 0)
    some = pl.ds(0, 3)
    rest = pl.ds(0, wide // 2)
    for way in range(2):
        landed(kv.at[some, 0], kg_s.at[way, 0])
        landed(kv.at[0, 0, pl.ds(0, 2)], kg_s.at[way, 1])
        landed(hz.at[some], hz_s.at[way, 0])
        landed(hz.at[0, :, rest], hz_s.at[way, 1])
        landed(xm.at[some, :, pl.ds(wide, half - wide)], ag_s.at[way, 0])
        landed(xm.at[0, :, pl.ds(wide, RING * len(ring_half[way]))], ag_s.at[way, 1])
        landed(ys.at[some, :, pl.ds(wide, half - wide)], rs_s.at[way, 0])
        landed(ys.at[0, :, pl.ds(wide, RING * len(ring_half[way]))], rs_s.at[way, 1])
        landed(cz.at[some], cr_s.at[way, 0])
        landed(cz.at[0, :, rest], cr_s.at[way, 1])
    landed(kv.at[:, 0], kx_s.at[0])
    landed(rz.at[pl.ds(0, 7)], rz_s.at[0])
    landed(xm, xs.at[0])
    landed(yps, yss.at[0])


def on_device(query, keys, values, residual, routes, gates, w_gate, w_up, w_down):
    _, tokens, half = query.shape
    units = w_gate.shape[2]
    kv_heads = keys.shape[2] // HD
    stacked = half // HD // kv_heads * tokens
    vmem = pl.BlockSpec(memory_space=pltpu.VMEM)
    hbm = pl.BlockSpec(memory_space=pl.ANY)
    dma = pltpu.SemaphoreType.DMA
    return pl.pallas_call(
        layer_kernel,
        out_shape=jax.ShapeDtypeStruct(query.shape, BF),
        in_specs=[hbm] * 4 + [vmem] * 2 + [hbm] * 3,
        out_specs=vmem,
        scratch_shapes=[
            pltpu.VMEM((tokens, half), BF),
            pltpu.VMEM((tokens, half), BF),
            pltpu.VMEM((8, 2, kv_heads, 2, tokens, HD), BF),
            pltpu.VMEM((kv_heads, stacked, HD), BF),
            pltpu.VMEM((kv_heads, stacked, 1), F32),
            pltpu.VMEM((kv_heads, stacked, HD), F32),
            pltpu.VMEM((kv_heads, stacked, HD), F32),
            pltpu.VMEM((tokens, half), BF),
            pltpu.VMEM((8, 8, 128), F32),
            pltpu.VMEM((8, MAIN, tokens), BF),
            pltpu.VMEM((8, EXPERTS, tokens), BF),
            pltpu.VMEM((8, MAIN, tokens), BF),
            pltpu.VMEM((8, MAIN, tokens), BF),
            pltpu.VMEM((8, EXPERTS, tokens), BF),
            pltpu.VMEM((8, EXPERTS, tokens), BF),
            pltpu.VMEM((8, tokens, WIDE), BF),
            pltpu.VMEM((2, half, units), BF),
            pltpu.VMEM((2, half, units), BF),
            pltpu.VMEM((2, units, half), BF),
            pltpu.VMEM((16, SLOTS, half - WIDE), BF),
            pltpu.VMEM((3, 8, 8, 128), F32),
            pltpu.VMEM((3, 8, 8, 128), F32),
            pltpu.VMEM((5, 16, 2, SLOTS, WIDE), BF),
            pltpu.VMEM((5, 8, 2, 8, 128), F32),
            pltpu.VMEM((5, 8, 2, 8, 128), F32),
            pltpu.VMEM((8, ROWS, half), BF),
            pltpu.VMEM((8, ROWS, half), BF),
            pltpu.VMEM((2, 2 * ROWS, units), F32),
            pltpu.VMEM((8 * ROWS, units), BF),
            pltpu.VMEM((8, ROWS, half), BF),
            pltpu.VMEM((8, ROWS, half), BF),
            pltpu.VMEM((8, ROWS, half), BF),
            pltpu.VMEM((2, 4, ROWS, half - WIDE), BF),
            pltpu.VMEM((3, 8, 8, 128), F32),
            pltpu.VMEM((16, SLOTS, half - WIDE), BF),
            pltpu.VMEM((3, 8, 8, 128), F32),
            pltpu.VMEM((5, 16, 2, SLOTS, WIDE), BF),
            pltpu.VMEM((5, 8, 2, 8, 128), F32),
            pltpu.VMEM((5, 8, 2, 8, 128), F32),
            pltpu.VMEM((8, tokens, WIDE), BF),
            pltpu.VMEM((2, 4, tokens, WIDE), BF),
            dma((3,)), dma((1,)), dma((1,)), dma((2, 2)), dma((2, 16)), dma((1,)), dma((8, 4)),
            dma((2, 2)), dma((2, 8)), dma((5,)), dma((5,)), dma((5,)), dma((5,)),
            dma((6,)), dma((3,)), dma((3,)), dma((3,)), dma((3,)),
            dma((2, 2)), dma((2, 20)), dma((1,)), dma((8, 3)), dma((1,)), dma((4, 4)),
            dma((2, 2)), dma((2, 20)), dma((3,)), dma((3,)), dma((3,)), dma((3,)),
            dma((5,)), dma((5,)), dma((5,)), dma((5,)), dma((2, 2)), dma((2, 8)),
        ],
        compiler_params=pltpu.CompilerParams(
            collective_id=1, has_side_effects=True, vmem_limit_bytes=60 * 1024 * 1024
        ),
        name="layer",
    )(query, keys, values, residual, routes[0].T, gates[0].T, w_gate, w_up, w_down)


def solution(mesh):
    return jax.shard_map(
        on_device,
        mesh=mesh,
        in_specs=(
            P("expert", "tensor", "section"),
            P("expert", "tensor", "section"),
            P("expert", "tensor", "section"),
            P("expert", "tensor", "section"),
            P("expert", "tensor", None),
            P("expert", "tensor", None),
            P("expert", None, "tensor"),
            P("expert", None, "tensor"),
            P("expert", "tensor", None),
        ),
        out_specs=P("expert", "tensor", "section"),
        check_vma=False,
    )
```

```python
import math

import jax
import jax.numpy as jnp
from jax import lax
from jax.experimental import pallas as pl
from jax.experimental.pallas import tpu as pltpu
from jax.sharding import PartitionSpec as P

HD = 128
EXPERTS = 8
NZ = 8
SLOTS = 8
MAIN = 2 * SLOTS * EXPERTS
ROWS = MAIN + EXPERTS
CHUNKS = 4
WIDE = 768
RING = 256
FAR = (0, 2, 4, 6, 5, 3, 1)
MESH = pl.DeviceIdType.MESH
BF = jnp.bfloat16
F32 = jnp.float32


def dot(a, b):
    return jnp.dot(a, b, preferred_element_type=F32)


def landed(ref, sem):
    pltpu.make_async_copy(ref, ref, sem).wait()


def dot_rows(a, b):
    return lax.dot_general(a, b, (((0,), (0,)), ((), ())), preferred_element_type=F32)


def copy_to(src, dst, send, recv, device):
    return pltpu.make_async_remote_copy(
        src_ref=src, dst_ref=dst, send_sem=send, recv_sem=recv, device_id=device, device_id_type=MESH
    )


def layer_kernel(
    q_any, k_any, v_any, res_any, routes, gates, wg_any, wu_any, wd_any, out,
    qv, res, kv, qs, top, mass, acc, hid, rz, hits, overs, high, low, ohigh, olow, hz,
    wg, wu, wd, pk, pov, ovr, pw, pvw, ovw, xm, xp, partial, inner, yps, ypr, ys, rr, fov, ret, retov,
    rb, pvb, ovb, cz, rc,
    in_sem, rz_s, rz_r, kg_s, kg_r, kx_s, kx_r, hz_s, hz_r, dw_s, dw_r, ow_s, ow_r,
    w_sem, d_s, d_r, o_s, o_r, ag_s, ag_r, xs, xrs, yss, yrs, rs_s, rs_r, b_s, b_r, bo_s, bo_r,
    bw_s, bw_r, vw_s, vw_r, cr_s, cr_r,
):
    s, e, t = lax.axis_index("section"), lax.axis_index("expert"), lax.axis_index("tensor")
    z, c = t // 2, t % 2
    tokens, half = hid.shape
    cw = half // CHUNKS
    kv_heads = qs.shape[0]
    own_in = []
    for h in range(kv_heads):
        at = pl.ds(HD * h, HD)
        own_in.append(pltpu.make_async_copy(k_any.at[0, :, at], kv.at[7, 0, h, 0], in_sem.at[0]))
        own_in.append(pltpu.make_async_copy(v_any.at[0, :, at], kv.at[7, 0, h, 1], in_sem.at[0]))
    queries_in = pltpu.make_async_copy(q_any.at[0], qv, in_sem.at[1])
    residual_in = pltpu.make_async_copy(res_any.at[0], res, in_sem.at[2])
    own_in += [queries_in, residual_in]
    for load in own_in:
        load.start()
    barrier = pltpu.get_barrier_semaphore()
    for i in range(1, 32):
        other = (s * 2 + c) ^ (i % 4)
        pl.semaphore_signal(
            barrier, inc=1, device_id=(other // 2, (e + i // 4) % 8, z * 2 + other % 2), device_id_type=MESH
        )
    up, down = (z + 1) % NZ, (z + NZ - 1) % NZ
    for k in range(1, NZ):
        pl.semaphore_signal(barrier, inc=1, device_id=(s, e, ((z + k) % NZ) * 2 + c), device_id_type=MESH)
    rz[7] = jnp.zeros(rz.shape[1:], F32)
    rz[7, 0:2, 0:tokens] = routes[...].astype(F32)
    rz[7, 2:4, 0:tokens] = gates[...]
    loads = []
    for part in range(2):
        h = (c + part) % 2
        rows = pl.ds(pl.multiple_of(h * half, half), half)
        loads.append(pltpu.make_async_copy(wg_any.at[0, rows, :], wg.at[part], w_sem.at[part]))
        loads.append(pltpu.make_async_copy(wu_any.at[0, rows, :], wu.at[part], w_sem.at[2 + part]))
        loads.append(pltpu.make_async_copy(wd_any.at[0, :, rows], wd.at[part], w_sem.at[4 + part]))

    def slot(way, d):
        return 7 if d == 0 else 6 if d == 4 else 2 * (d - 1) + way

    partner = (s, e, z * 2 + 1 - c)
    ring = ((s, e, up * 2 + c), (s, e, down * 2 + c))

    def spread(way, d, h):
        return copy_to(
            kv.at[slot(way, d), 0, h], kv.at[slot(way, d + 1), 0, h],
            kg_s.at[way, d // 3], kg_r.at[way, 4 * d + h], ring[way],
        )

    def swap(k, h):
        return copy_to(kv.at[k, 0, h], kv.at[k, 1, h], kx_s.at[0], kx_r.at[k, h], partner)

    tell = [
        copy_to(rz.at[7], rz.at[FAR[k - 1]], rz_s.at[0], rz_r.at[0], (s, e, ((z + k) % NZ) * 2 + c))
        for k in range(1, NZ)
    ]
    landed(kv.at[7, 0], in_sem.at[0])
    pl.semaphore_wait(barrier, 38)
    for h in range(kv_heads):
        for way in range(2):
            spread(way, 0, h).start()
        swap(7, h).start()
    for copy in tell:
        copy.start()
    for load in loads:
        load.start()

    earlier = (
        lax.broadcasted_iota(jnp.int32, (tokens, tokens), 0) < lax.broadcasted_iota(jnp.int32, (tokens, tokens), 1)
    ).astype(BF)

    line = lax.broadcasted_iota(jnp.int32, (MAIN, tokens), 0)
    few = lax.broadcasted_iota(jnp.int32, (EXPERTS, tokens), 0)

    def placed(k, expert, wanted, hit_ref, high_ref, low_ref):
        is0, is1 = (rz[k, n : n + 1, 0:tokens] == expert.astype(F32) for n in range(2))
        gate0, gate1 = (rz[k, n : n + 1, 0:tokens] for n in (2, 3))
        named = jnp.where(is0 | is1, 1.0, 0.0)
        place = dot(named.astype(BF), earlier)
        hit = jnp.where(place == wanted.astype(F32), named, 0.0)
        weight = hit * (jnp.where(is0, gate0, 0.0) + jnp.where(is1, gate1, 0.0))
        top_part = weight.astype(BF)
        hit_ref[k] = hit.astype(BF)
        high_ref[k] = top_part
        low_ref[k] = (weight - top_part.astype(F32)).astype(BF)

    def slot_tables(k):
        placed(k, line // (2 * SLOTS), line % (2 * SLOTS), hits, high, low)
        placed(k, few, jnp.full_like(few, 2 * SLOTS), overs, ohigh, olow)

    slot_tables(7)
    queries_in.wait()
    group = qs.shape[1] // tokens
    for h in range(kv_heads):
        for g in range(group):
            qs[h, tokens * g : tokens * (g + 1), :] = qv[:, HD * (h * group + g) : HD * (h * group + g + 1)]
    stacked = group * tokens
    scale = math.log2(math.e) / math.sqrt(HD)

    def attend(start, count, bias, fresh, h):
        keys = count * 2 * tokens
        k = kv[start : start + count, :, h, 0].reshape(keys, HD)
        v = kv[start : start + count, :, h, 1].reshape(keys, HD)
        scores = lax.dot_general(qs[h], k, (((1,), (1,)), ((), ())), preferred_element_type=F32) * scale + bias
        peak = jnp.max(scores, axis=1, keepdims=True)
        if not fresh:
            peak = jnp.maximum(peak, top[h])
        terms = jnp.exp2(scores - peak).astype(BF)
        both = dot(terms, jnp.concatenate([v, jnp.ones_like(v)], axis=1))
        context, total = both[:, :HD], both[:, HD:]
        if not fresh:
            fade = jnp.exp2(top[h] - peak)
            total = total + mass[h] * fade
            context = context + acc[h] * fade
        top[h], mass[h], acc[h] = peak, total, context

    row = lax.broadcasted_iota(jnp.int32, (stacked, 2 * tokens), 0) % tokens
    col = lax.broadcasted_iota(jnp.int32, (stacked, 2 * tokens), 1)
    diagonal = jnp.where(col <= jnp.where(col < tokens, row, jnp.where(c == 1, 2 * tokens, -1)), 0.0, -1e30)

    def ring_bias(d):
        col = lax.broadcasted_iota(jnp.int32, (1, (2 if d < 4 else 1) * 2 * tokens), 1)
        return jnp.where(jnp.where(col < 2 * tokens, z - d, z + d - NZ) >= 0, 0.0, -1e30)

    def first_step(h, carry):
        swap(7, h).wait_recv()
        attend(7, 1, diagonal, True, h)
        return carry

    lax.fori_loop(0, kv_heads, first_step, 0)
    for d in range(1, 4):
        bias = ring_bias(d - 1) if d > 1 else None

        def ring_step(h, carry, d=d, bias=bias):
            for way in range(2):
                spread(way, d - 1, h).wait_recv()
                if d < 3:
                    spread(way, d, h).start()
                else:
                    pl.when(h // 2 == way)(spread(way, d, h).start)
                swap(slot(way, d), h).start()
            if d > 1:
                for way in range(2):
                    swap(slot(way, d - 1), h).wait_recv()
                attend(slot(0, d - 1), 2, bias, False, h)
            return carry

        lax.fori_loop(0, kv_heads, ring_step, 0)
    bias = ring_bias(3)

    def last_step(h, carry):
        for way in range(2):
            swap(slot(way, 3), h).wait_recv()
        attend(slot(0, 3), 2, bias, False, h)
        return carry

    bias4 = ring_bias(4)
    landed(rz.at[pl.ds(0, 7)], rz_r.at[0])
    for k in range(7):
        slot_tables(k)
    for h in range(2):
        last_step(h, 0)
        for way in range(2):
            spread(way, 3, 2 * way + h).wait_recv()
            swap(6, 2 * way + h).start()
    residual_in.wait()

    own = s == c
    wide = WIDE
    rings = (half - wide) // RING
    ring_half = (tuple(range((rings + 1) // 2)), tuple(range((rings + 1) // 2, rings)))
    hw = half // kv_heads

    def ring_cols(j):
        return pl.ds(wide + RING * j, RING)

    def send(copy, i, same):
        if i == 0 and same:
            pl.when(jnp.logical_not(own))(copy.start)
        else:
            copy.start()

    def settle(ref, sem, axis):
        index = [slice(None)] * len(ref.shape)
        index[axis] = pl.ds(0, ref.shape[axis] - ref.shape[axis] // (16 if ref.shape[axis] > 8 else 8))
        fewer = tuple(pl.ds(0, n) if isinstance(i, slice) else i for i, n in zip(index, ref.shape))

        @pl.when(own)
        def _():
            landed(ref.at[fewer], sem)

        @pl.when(jnp.logical_not(own))
        def _():
            landed(ref, sem)

    def source_rows(ef, cf):
        return pl.ds(pl.multiple_of((ef * 2 + cf) * SLOTS, SLOTS), SLOTS)

    carry_on = {}
    for way in range(2):
        for d in range(4):
            for j in range(2) if d < 3 else (way,):
                at = pl.ds(wide // 2 * j, wide // 2)
                carry_on[way, d, j] = copy_to(
                    hz.at[slot(way, d), :, at], hz.at[slot(way, d + 1), :, at],
                    hz_s.at[way, d // 3], hz_r.at[way, 2 * d + j], ring[way],
                )

    for h in range(kv_heads):
        swap(6, h).wait_recv()
        if h >= 2:
            last_step(h, 0)
        attend(6, 1, bias4, False, h)
        context = acc[h] / mass[h]
        for g in range(group):
            at = slice(HD * (h * group + g), HD * (h * group + g + 1))
            hid[:, at] = (res[:, at].astype(F32) + context[tokens * g : tokens * (g + 1), :]).astype(BF)
        from_col = hw * h
        if from_col < wide:
            to_col = min(wide, from_col + hw)
            hz[7, :, from_col:to_col] = hid[:, from_col:to_col]
            for j in range(2):
                if from_col < wide // 2 * (j + 1) <= to_col:
                    for way in range(2):
                        carry_on[way, 0, j].start()
        if h == 0:
            continue
        a = h - 1
        from_col = max(from_col, wide)
        width = hw * (h + 1) - from_col
        piece = hid[:, from_col : from_col + width]
        part = pl.ds(from_col - wide, width)
        pk[:, :, part] = dot(hits[7], piece).astype(BF).reshape(16, SLOTS, width)
        extra = dot(overs[7], piece)
        for q in range(width // 128):
            pov[a, :, q, :] = extra[:, 128 * q : 128 * (q + 1)]
        land = pl.ds(from_col, width)

        @pl.when(own)
        def _():
            xm[7, source_rows(e, c), land] = pk[e * 2 + s, :, part]
            ovr[a, e] = pov[a, e]

        for i in range(8):
            ed = (e + i) % 8
            for k in (1, 0):
                sd = (s + k) % 2
                send(
                    copy_to(
                        pk.at[ed * 2 + sd, :, part], xm.at[7, source_rows(e, c), land],
                        d_s.at[a], d_r.at[a], (sd, ed, z * 2 + s),
                    ), i, k == 0,
                )
            send(copy_to(pov.at[a, ed], ovr.at[a, e], o_s.at[a], o_r.at[a], (c, ed, z * 2 + s)), i, True)

    groups = ((7, 1), (0, 2), (2, 2), (4, 2), (6, 1))

    def send_wide(w):
        start, count = groups[w]
        for p in range(count):
            tokens_of = hz[start + p]
            pw[w, :, p] = dot(hits[start + p], tokens_of).astype(BF).reshape(16, SLOTS, wide)
            extra = dot(overs[start + p], tokens_of)
            for q in range(wide // 128):
                pvw[w, :, p, q, :] = extra[:, 128 * q : 128 * (q + 1)]
        many = pl.ds(0, count)
        slots = pl.ds(start, count)
        at = pl.ds(0, wide)

        @pl.when(own)
        def _():
            xm[slots, source_rows(e, c), at] = pw[w, e * 2 + s, many]
            ovw[w, e, many] = pvw[w, e, many]

        for i in range(8):
            ed = (e + i) % 8
            for k in (1, 0):
                sd = (s + k) % 2
                send(
                    copy_to(
                        pw.at[w, ed * 2 + sd, many], xm.at[slots, source_rows(e, c), at],
                        dw_s.at[w], dw_r.at[w], (sd, ed, z * 2 + s),
                    ), i, k == 0,
                )
            send(
                copy_to(pvw.at[w, ed, many], ovw.at[w, e, many], ow_s.at[w], ow_r.at[w], (c, ed, z * 2 + s)),
                i, True,
            )

    def receive_wide(w):
        start, count = groups[w]
        many = pl.ds(0, count)
        slots = pl.ds(start, count)
        at = pl.ds(0, wide)
        settle(xm.at[slots, pl.ds(0, MAIN), at], dw_r.at[w], 1)
        settle(ovw.at[w, :, many], ow_r.at[w], 0)
        for p in range(count):
            for q in range(wide // 128):
                xm[start + p, MAIN:, 128 * q : 128 * (q + 1)] = ovw[w, :, p, q, :].astype(BF)
            share[start + p, 0].start()

    def carry(d):
        for j in range(2):
            for way in range(2) if d < 4 else (j,):
                carry_on[way, d - 1, j].wait_recv()
                if (way, d, j) in carry_on:
                    carry_on[way, d, j].start()

    def cols(j):
        return pl.ds(cw * j, cw)

    half_of = ((0, 1), (2, 3))
    gather, share = {}, {}
    split = wide + 3 * RING
    parts = ((0, wide), (wide, split), (split, half))
    for way in range(2):
        for d in range(4):
            for j in range(rings) if d < 3 else ring_half[way]:
                n = d * rings + j
                gather[way, d, j] = copy_to(
                    xm.at[slot(way, d), :, ring_cols(j)], xm.at[slot(way, d + 1), :, ring_cols(j)],
                    ag_s.at[way, d // 3], ag_r.at[way, n], ring[way],
                )
    for k in range(8):
        for n, (begin, end) in enumerate(parts):
            at = pl.ds(begin, end - begin)
            share[k, n] = copy_to(xm.at[k, :, at], xp.at[k, :, at], xs.at[0], xrs.at[k, n], partner)

    def trade(g, j):
        at = pl.ds(pl.multiple_of(j * cw, cw), cw)
        pair = pl.ds(2 * g - 2, 2)
        return copy_to(yps.at[pair, :, at], ypr.at[pair, :, at], yss.at[0], yrs.at[g - 1, j], partner)

    def hidden_units(g, first, last):
        def piece(k, carry):
            at = pl.ds(pl.multiple_of(k * 256, 256), 256)
            left = xm[2 * g - 2 : 2 * g].reshape(2 * ROWS, half)
            right = xp[2 * g - 2 : 2 * g].reshape(2 * ROWS, half)
            gate = dot(left, wg[0, :, at]) + dot(right, wg[1, :, at])
            lift = dot(left, wu[0, :, at]) + dot(right, wu[1, :, at])
            inner[pl.ds((2 * g - 2) * ROWS, 2 * ROWS), at] = (gate / (1.0 + jnp.exp(-gate)) * lift).astype(BF)
            return carry

        lax.fori_loop(first, last, piece, 0)

    def units_part(g, n, fresh, done):
        begin, end = parts[n]
        at_k = pl.ds(begin, end - begin)

        def piece(k, carry):
            at = pl.ds(pl.multiple_of(k * 256, 256), 256)
            left = xm[2 * g - 2 : 2 * g, :, at_k].reshape(2 * ROWS, end - begin)
            right = xp[2 * g - 2 : 2 * g, :, at_k].reshape(2 * ROWS, end - begin)
            gate = dot(left, wg[0, at_k, at]) + dot(right, wg[1, at_k, at])
            lift = dot(left, wu[0, at_k, at]) + dot(right, wu[1, at_k, at])
            if not fresh:
                gate, lift = gate + partial[0, :, at], lift + partial[1, :, at]
            if done:
                inner[pl.ds((2 * g - 2) * ROWS, 2 * ROWS), at] = (gate / (1.0 + jnp.exp(-gate)) * lift).astype(BF)
            else:
                partial[0, :, at], partial[1, :, at] = gate, lift
            return carry

        lax.fori_loop(0, 2, piece, 0)

    def down_out(g):
        rows = inner[pl.ds((2 * g - 2) * ROWS, 2 * ROWS), :]

        def theirs(j, carry):
            at = pl.ds(pl.multiple_of(j * cw, cw), cw)
            yps[pl.ds(2 * g - 2, 2), :, at] = dot(rows, wd[1, :, at]).astype(BF).reshape(2, ROWS, cw)
            trade(g, j).start()
            return carry

        lax.fori_loop(0, CHUNKS, theirs, 0)

    def down_own(g):
        rows = inner[pl.ds((2 * g - 2) * ROWS, 2 * ROWS), :]

        def mine(j, carry):
            trade(g, j).wait_recv()
            at = pl.ds(pl.multiple_of(j * cw, cw), cw)
            both = dot(rows, wd[0, :, at]).reshape(2, ROWS, cw) + ypr[pl.ds(2 * g - 2, 2), :, at].astype(F32)
            ys[pl.ds(2 * g - 2, 2), :, at] = both.astype(BF)
            return carry

        lax.fori_loop(0, CHUNKS, mine, 0)

    reduce, link = {}, {}
    for way in range(2):
        for d in range(1, 5):
            target = slot(1 - way, d)
            for j in range(rings) if d < 4 else ring_half[way]:
                n = (d - 1) * rings + j
                reduce[way, d, j] = copy_to(
                    ys.at[target, :, ring_cols(j)], rr.at[way, d - 1, :, pl.ds(RING * j, RING)],
                    rs_s.at[way, d // 4], rs_r.at[way, n], ring[way],
                )
            for j in range(2) if d < 4 else (way,):
                at = pl.ds(wide // 2 * j, wide // 2)
                link[way, d, j] = copy_to(
                    cz.at[target, :, at], rc.at[way, d - 1, :, at],
                    cr_s.at[way, d // 4], cr_r.at[way, 2 * (d - 1) + j], ring[way],
                )

    def pass_on(way, d, j, add):
        if add:
            reduce[way, d + 1, j].wait_recv()
            k = slot(1 - way, d)
            total = ys[k, :, ring_cols(j)].astype(F32) + rr[way, d, :, pl.ds(RING * j, RING)].astype(F32)
            ys[k, :, ring_cols(j)] = total.astype(BF)
        reduce[way, d, j].start()

    def both_ways(d, lists, add):
        for n in range(max(len(lists[0]), len(lists[1]))):
            for way in range(2):
                if n < len(lists[way]):
                    pass_on(way, d, lists[way][n], add)

    def chain(d):
        for j in range(2):
            at = pl.ds(wide // 2 * j, wide // 2)
            for way in range(2):
                if (way, d, j) in link:
                    if (way, d + 1, j) in link:
                        link[way, d + 1, j].wait_recv()
                        k = slot(1 - way, d)
                        cz[k, :, at] = (cz[k, :, at].astype(F32) + rc[way, d, :, at].astype(F32)).astype(BF)
                    link[way, d, j].start()

    def weigh(k, rows, extra):
        return (
            dot_rows(high[k], rows) + dot_rows(low[k], rows) + dot_rows(ohigh[k], extra) + dot_rows(olow[k], extra)
        )

    def send_back(w):
        start, count = groups[w]
        many, slots, at = pl.ds(0, count), pl.ds(start, count), pl.ds(0, wide)
        for p in range(count):
            tail = ys[start + p, MAIN:, at].astype(F32)
            for q in range(wide // 128):
                pvb[w, :, p, q, :] = tail[:, 128 * q : 128 * (q + 1)]

        @pl.when(own)
        def _():
            rb[w, e * 2 + s, many] = ys[slots, source_rows(e, c), at]
            ovb[w, e, many] = pvb[w, e, many]

        for i in range(8):
            ed = (e + i) % 8
            for k in (1, 0):
                cd = (c + k) % 2
                send(
                    copy_to(
                        ys.at[slots, source_rows(ed, cd), at], rb.at[w, e * 2 + s, many],
                        bw_s.at[w], bw_r.at[w], (c, ed, z * 2 + cd),
                    ), i, k == 0,
                )
            send(
                copy_to(pvb.at[w, ed, many], ovb.at[w, e, many], vw_s.at[w], vw_r.at[w], (c, ed, z * 2 + s)),
                i, True,
            )

    def receive_back(w):
        start, count = groups[w]
        many, slots, at = pl.ds(0, count), pl.ds(start, count), pl.ds(0, wide)
        settle(rb.at[w, :, many], bw_r.at[w], 0)
        settle(ovb.at[w, :, many], vw_r.at[w], 0)
        totals = []
        for p in range(count):
            extra = jnp.concatenate([ovb[w, :, p, q, :] for q in range(wide // 128)], axis=1).astype(BF)
            totals.append(weigh(start + p, rb[w, :, p].reshape(MAIN, wide), extra))
            if w > 0:
                cz[start + p] = totals[p].astype(BF)
        return totals[0]

    send_wide(0)
    carry(1)
    send_wide(1)
    for a in range(3):
        from_col = max(wide, hw * (a + 1))
        width = hw * (a + 2) - from_col
        land = pl.ds(from_col, width)
        part = pl.ds(from_col - wide, width)
        settle(xm.at[7, pl.ds(0, MAIN), land], d_r.at[a], 0)
        settle(ovr.at[a], o_r.at[a], 0)
        for q in range(width // 128):
            at = from_col + 128 * q
            xm[7, MAIN:, at : at + 128] = ovr[a, :, q, :].astype(BF)
        for j in range((from_col - wide) // RING, (from_col - wide + width) // RING):
            for way in range(2):
                gather[way, 0, j].start()
        if a == 1:
            carry(2)
    share[7, 1].start()
    share[7, 2].start()
    send_wide(2)
    carry(3)
    send_wide(3)
    for load in loads:
        load.wait()

    receive_wide(0)

    def shared(k):
        for n in range(3):
            share[k, n].wait_recv()

    for d in range(1, 4):
        if d > 1:
            receive_wide(d - 1)
            for way in range(2):
                shared(slot(way, d - 1))
        for j in range(rings):
            for way in range(2):
                gather[way, d - 1, j].wait_recv()
                if (way, d, j) in gather:
                    gather[way, d, j].start()
                if j in (2, rings - 1):
                    share[slot(way, d), 1 + j // 3].start()
            if d == 1 and j == 1:
                carry(4)
                send_wide(4)
            if d > 1 and j in (1, 3):
                hidden_units(d - 1, j // 2, j // 2 + 1)
            if d == 3 and j == 2:
                receive_wide(3)
            if d == 3 and j == 3:
                for way in range(2):
                    share[slot(way, 3), 1].wait_recv()
                units_part(3, 1, True, False)
    receive_wide(4)
    for way in range(2):
        share[slot(way, 3), 2].wait_recv()
    units_part(3, 2, False, False)
    for way in range(2):
        share[slot(way, 3), 0].wait_recv()
    units_part(3, 0, False, True)
    down_out(3)
    for way in range(2):
        for j in ring_half[way]:
            gather[way, 3, j].wait_recv()
    share[6, 1].start()
    share[6, 2].start()
    down_own(3)

    swapped = (ring_half[1], ring_half[0])
    orders = tuple(b + a for a, b in zip(ring_half, swapped))
    lasts = (orders[0], (0, 3, 4, 1, 2))
    both_ways(3, swapped, False)
    send_back(3)
    down_out(2)
    shared(6)
    shared(7)
    hidden_units(4, 0, 2)
    down_out(4)
    down_own(2)
    both_ways(2, swapped, True)
    down_own(4)
    both_ways(4, ring_half, False)
    send_back(4)
    send_back(2)
    down_out(1)
    receive_back(3)
    both_ways(3, ring_half, True)
    receive_back(4)
    chain(4)
    down_own(1)
    send_back(1)
    send_back(0)
    both_ways(2, ring_half, True)
    chain(3)
    receive_back(2)
    both_ways(1, tuple(o[:2] for o in lasts), True)
    chain(2)
    receive_back(1)
    both_ways(1, tuple(o[2:4] for o in lasts), True)
    both_ways(1, tuple(o[4:] for o in lasts), True)
    chain(1)

    pieces = ((3, 2), (0, 2), (2, 1))
    for a, (j, count) in enumerate(pieces):
        width = count * RING
        for n in range(j, j + count):
            for way in range(2):
                reduce[way, 1, n].wait_recv()
        land, part = pl.ds(wide + RING * j, width), pl.ds(RING * j, width)
        total = (
            ys[7, :, land].astype(F32) + rr[0, 0, :, part].astype(F32) + rr[1, 0, :, part].astype(F32)
        ).astype(BF)
        ys[7, :, land] = total
        tail = total[MAIN:].astype(F32)
        for q in range(width // 128):
            fov[a, :, q, :] = tail[:, 128 * q : 128 * (q + 1)]

        @pl.when(own)
        def _():
            ret[e * 2 + s, :, part] = ys[7, source_rows(e, c), land]
            retov[a, e] = fov[a, e]

        for i in range(8):
            ed = (e + i) % 8
            for k in (1, 0):
                cd = (c + k) % 2
                send(
                    copy_to(
                        ys.at[7, source_rows(ed, cd), land], ret.at[e * 2 + s, :, part],
                        b_s.at[a], b_r.at[a], (c, ed, z * 2 + cd),
                    ), i, k == 0,
                )
            send(copy_to(fov.at[a, ed], retov.at[a, e], bo_s.at[a], bo_r.at[a], (c, ed, z * 2 + s)), i, True)

    total = receive_back(0)
    for way in range(2):
        for j in range(2):
            link[way, 1, j].wait_recv()
        total = total + rc[way, 0].astype(F32)
    out[0, :, 0:wide] = (hid[:, 0:wide].astype(F32) + total).astype(BF)

    for a, (j, count) in enumerate(pieces):
        width = count * RING
        land, part = pl.ds(wide + RING * j, width), pl.ds(RING * j, width)
        settle(ret.at[:, :, part], b_r.at[a], 0)
        settle(retov.at[a], bo_r.at[a], 0)
        extra = jnp.concatenate([retov[a, :, q, :] for q in range(width // 128)], axis=1).astype(BF)
        total = weigh(7, ret[:, :, part].reshape(MAIN, width), extra)
        out[0, :, land] = (hid[:, land].astype(F32) + total).astype(BF)

    for a in range(3):
        from_col = max(wide, hw * (a + 1))
        part = pl.ds(from_col - wide, hw * (a + 2) - from_col)
        settle(pk.at[:, :, part], d_s.at[a], 0)
        settle(pov.at[a], o_s.at[a], 0)
        settle(ret.at[:, :, pl.ds(RING * pieces[a][0], RING * pieces[a][1])], b_s.at[a], 0)
        settle(fov.at[a], bo_s.at[a], 0)
    for w, (start, count) in enumerate(groups):
        many = pl.ds(0, count)
        settle(pw.at[w, :, many], dw_s.at[w], 0)
        settle(pvw.at[w, :, many], ow_s.at[w], 0)
        settle(rb.at[w, :, many], bw_s.at[w], 0)
        settle(pvb.at[w, :, many], vw_s.at[w], 0)
    some = pl.ds(0, 3)
    rest = pl.ds(0, wide // 2)
    for way in range(2):
        landed(kv.at[some, 0], kg_s.at[way, 0])
        landed(kv.at[0, 0, pl.ds(0, 2)], kg_s.at[way, 1])
        landed(hz.at[some], hz_s.at[way, 0])
        landed(hz.at[0, :, rest], hz_s.at[way, 1])
        landed(xm.at[some, :, pl.ds(wide, half - wide)], ag_s.at[way, 0])
        landed(xm.at[0, :, pl.ds(wide, RING * len(ring_half[way]))], ag_s.at[way, 1])
        landed(ys.at[some, :, pl.ds(wide, half - wide)], rs_s.at[way, 0])
        landed(ys.at[0, :, pl.ds(wide, RING * len(ring_half[way]))], rs_s.at[way, 1])
        landed(cz.at[some], cr_s.at[way, 0])
        landed(cz.at[0, :, rest], cr_s.at[way, 1])
    landed(kv.at[:, 0], kx_s.at[0])
    landed(rz.at[pl.ds(0, 7)], rz_s.at[0])
    landed(xm, xs.at[0])
    landed(yps, yss.at[0])


def on_device(query, keys, values, residual, routes, gates, w_gate, w_up, w_down):
    _, tokens, half = query.shape
    units = w_gate.shape[2]
    kv_heads = keys.shape[2] // HD
    stacked = half // HD // kv_heads * tokens
    vmem = pl.BlockSpec(memory_space=pltpu.VMEM)
    hbm = pl.BlockSpec(memory_space=pl.ANY)
    dma = pltpu.SemaphoreType.DMA
    return pl.pallas_call(
        layer_kernel,
        out_shape=jax.ShapeDtypeStruct(query.shape, BF),
        in_specs=[hbm] * 4 + [vmem] * 2 + [hbm] * 3,
        out_specs=vmem,
        scratch_shapes=[
            pltpu.VMEM((tokens, half), BF),
            pltpu.VMEM((tokens, half), BF),
            pltpu.VMEM((8, 2, kv_heads, 2, tokens, HD), BF),
            pltpu.VMEM((kv_heads, stacked, HD), BF),
            pltpu.VMEM((kv_heads, stacked, 1), F32),
            pltpu.VMEM((kv_heads, stacked, HD), F32),
            pltpu.VMEM((kv_heads, stacked, HD), F32),
            pltpu.VMEM((tokens, half), BF),
            pltpu.VMEM((8, 8, 128), F32),
            pltpu.VMEM((8, MAIN, tokens), BF),
            pltpu.VMEM((8, EXPERTS, tokens), BF),
            pltpu.VMEM((8, MAIN, tokens), BF),
            pltpu.VMEM((8, MAIN, tokens), BF),
            pltpu.VMEM((8, EXPERTS, tokens), BF),
            pltpu.VMEM((8, EXPERTS, tokens), BF),
            pltpu.VMEM((8, tokens, WIDE), BF),
            pltpu.VMEM((2, half, units), BF),
            pltpu.VMEM((2, half, units), BF),
            pltpu.VMEM((2, units, half), BF),
            pltpu.VMEM((16, SLOTS, half - WIDE), BF),
            pltpu.VMEM((3, 8, 8, 128), F32),
            pltpu.VMEM((3, 8, 8, 128), F32),
            pltpu.VMEM((5, 16, 2, SLOTS, WIDE), BF),
            pltpu.VMEM((5, 8, 2, 8, 128), F32),
            pltpu.VMEM((5, 8, 2, 8, 128), F32),
            pltpu.VMEM((8, ROWS, half), BF),
            pltpu.VMEM((8, ROWS, half), BF),
            pltpu.VMEM((2, 2 * ROWS, units), F32),
            pltpu.VMEM((8 * ROWS, units), BF),
            pltpu.VMEM((8, ROWS, half), BF),
            pltpu.VMEM((8, ROWS, half), BF),
            pltpu.VMEM((8, ROWS, half), BF),
            pltpu.VMEM((2, 4, ROWS, half - WIDE), BF),
            pltpu.VMEM((3, 8, 8, 128), F32),
            pltpu.VMEM((16, SLOTS, half - WIDE), BF),
            pltpu.VMEM((3, 8, 8, 128), F32),
            pltpu.VMEM((5, 16, 2, SLOTS, WIDE), BF),
            pltpu.VMEM((5, 8, 2, 8, 128), F32),
            pltpu.VMEM((5, 8, 2, 8, 128), F32),
            pltpu.VMEM((8, tokens, WIDE), BF),
            pltpu.VMEM((2, 4, tokens, WIDE), BF),
            dma((3,)), dma((1,)), dma((1,)), dma((2, 2)), dma((2, 16)), dma((1,)), dma((8, 4)),
            dma((2, 2)), dma((2, 8)), dma((5,)), dma((5,)), dma((5,)), dma((5,)),
            dma((6,)), dma((3,)), dma((3,)), dma((3,)), dma((3,)),
            dma((2, 2)), dma((2, 20)), dma((1,)), dma((8, 3)), dma((1,)), dma((4, 4)),
            dma((2, 2)), dma((2, 20)), dma((3,)), dma((3,)), dma((3,)), dma((3,)),
            dma((5,)), dma((5,)), dma((5,)), dma((5,)), dma((2, 2)), dma((2, 8)),
        ],
        compiler_params=pltpu.CompilerParams(
            collective_id=1, has_side_effects=True, vmem_limit_bytes=60 * 1024 * 1024
        ),
        name="layer",
    )(query, keys, values, residual, routes[0].T, gates[0].T, w_gate, w_up, w_down)


def solution(mesh):
    return jax.shard_map(
        on_device,
        mesh=mesh,
        in_specs=(
            P("expert", "tensor", "section"),
            P("expert", "tensor", "section"),
            P("expert", "tensor", "section"),
            P("expert", "tensor", "section"),
            P("expert", "tensor", None),
            P("expert", "tensor", None),
            P("expert", None, "tensor"),
            P("expert", None, "tensor"),
            P("expert", "tensor", None),
        ),
        out_specs=P("expert", "tensor", "section"),
        check_vma=False,
    )
```

```python
import math

import jax
import jax.numpy as jnp
from jax import lax
from jax.experimental import pallas as pl
from jax.experimental.pallas import tpu as pltpu
from jax.sharding import PartitionSpec as P

HD = 128
EXPERTS = 8
NZ = 8
SLOTS = 8
MAIN = 2 * SLOTS * EXPERTS
ROWS = MAIN + EXPERTS
CHUNKS = 4
WIDE = 768
RING = 256
FAR = (0, 2, 4, 6, 5, 3, 1)
MESH = pl.DeviceIdType.MESH
BF = jnp.bfloat16
F32 = jnp.float32


def dot(a, b):
    return jnp.dot(a, b, preferred_element_type=F32)


def landed(ref, sem):
    pltpu.make_async_copy(ref, ref, sem).wait()


def dot_rows(a, b):
    return lax.dot_general(a, b, (((0,), (0,)), ((), ())), preferred_element_type=F32)


def copy_to(src, dst, send, recv, device):
    return pltpu.make_async_remote_copy(
        src_ref=src, dst_ref=dst, send_sem=send, recv_sem=recv, device_id=device, device_id_type=MESH
    )


def layer_kernel(
    q_any, k_any, v_any, res_any, routes, gates, wg_any, wu_any, wd_any, out,
    qv, res, kv, qs, top, mass, acc, hid, rz, hits, overs, high, low, ohigh, olow, hz,
    wg, wu, wd, pk, pov, ovr, pw, pvw, ovw, xm, xp, partial, inner, yps, ypr, ys, rr, fov, ret, retov,
    rb, pvb, ovb, cz, rc,
    in_sem, rz_s, rz_r, kg_s, kg_r, kx_s, kx_r, hz_s, hz_r, dw_s, dw_r, ow_s, ow_r,
    w_sem, d_s, d_r, o_s, o_r, ag_s, ag_r, xs, xrs, yss, yrs, rs_s, rs_r, b_s, b_r, bo_s, bo_r,
    bw_s, bw_r, vw_s, vw_r, cr_s, cr_r,
):
    s, e, t = lax.axis_index("section"), lax.axis_index("expert"), lax.axis_index("tensor")
    z, c = t // 2, t % 2
    tokens, half = hid.shape
    cw = half // CHUNKS
    kv_heads = qs.shape[0]
    own_in = []
    for h in range(kv_heads):
        at = pl.ds(HD * h, HD)
        own_in.append(pltpu.make_async_copy(k_any.at[0, :, at], kv.at[7, 0, h, 0], in_sem.at[0]))
        own_in.append(pltpu.make_async_copy(v_any.at[0, :, at], kv.at[7, 0, h, 1], in_sem.at[0]))
    queries_in = pltpu.make_async_copy(q_any.at[0], qv, in_sem.at[1])
    residual_in = pltpu.make_async_copy(res_any.at[0], res, in_sem.at[2])
    own_in += [queries_in, residual_in]
    for load in own_in:
        load.start()
    barrier = pltpu.get_barrier_semaphore()
    for i in range(1, 32):
        other = (s * 2 + c) ^ (i % 4)
        pl.semaphore_signal(
            barrier, inc=1, device_id=(other // 2, (e + i // 4) % 8, z * 2 + other % 2), device_id_type=MESH
        )
    up, down = (z + 1) % NZ, (z + NZ - 1) % NZ
    for k in range(1, NZ):
        pl.semaphore_signal(barrier, inc=1, device_id=(s, e, ((z + k) % NZ) * 2 + c), device_id_type=MESH)
    rz[7] = jnp.zeros(rz.shape[1:], F32)
    rz[7, 0:2, 0:tokens] = routes[...].astype(F32)
    rz[7, 2:4, 0:tokens] = gates[...]
    loads = []
    for part in range(2):
        h = (c + part) % 2
        rows = pl.ds(pl.multiple_of(h * half, half), half)
        loads.append(pltpu.make_async_copy(wg_any.at[0, rows, :], wg.at[part], w_sem.at[part]))
        loads.append(pltpu.make_async_copy(wu_any.at[0, rows, :], wu.at[part], w_sem.at[2 + part]))
        loads.append(pltpu.make_async_copy(wd_any.at[0, :, rows], wd.at[part], w_sem.at[4 + part]))

    def slot(way, d):
        return 7 if d == 0 else 6 if d == 4 else 2 * (d - 1) + way

    partner = (s, e, z * 2 + 1 - c)
    ring = ((s, e, up * 2 + c), (s, e, down * 2 + c))

    def spread(way, d, h):
        return copy_to(
            kv.at[slot(way, d), 0, h], kv.at[slot(way, d + 1), 0, h],
            kg_s.at[way, d // 3], kg_r.at[way, 4 * d + h], ring[way],
        )

    def swap(k, h):
        return copy_to(kv.at[k, 0, h], kv.at[k, 1, h], kx_s.at[0], kx_r.at[k, h], partner)

    tell = [
        copy_to(rz.at[7], rz.at[FAR[k - 1]], rz_s.at[0], rz_r.at[0], (s, e, ((z + k) % NZ) * 2 + c))
        for k in range(1, NZ)
    ]
    landed(kv.at[7, 0], in_sem.at[0])
    pl.semaphore_wait(barrier, 38)
    for h in range(kv_heads):
        for way in range(2):
            spread(way, 0, h).start()
        swap(7, h).start()
    for copy in tell:
        copy.start()
    for load in loads:
        load.start()

    earlier = (
        lax.broadcasted_iota(jnp.int32, (tokens, tokens), 0) < lax.broadcasted_iota(jnp.int32, (tokens, tokens), 1)
    ).astype(BF)

    line = lax.broadcasted_iota(jnp.int32, (MAIN, tokens), 0)
    few = lax.broadcasted_iota(jnp.int32, (EXPERTS, tokens), 0)

    def placed(k, expert, wanted, hit_ref, high_ref, low_ref):
        is0, is1 = (rz[k, n : n + 1, 0:tokens] == expert.astype(F32) for n in range(2))
        gate0, gate1 = (rz[k, n : n + 1, 0:tokens] for n in (2, 3))
        named = jnp.where(is0 | is1, 1.0, 0.0)
        place = dot(named.astype(BF), earlier)
        hit = jnp.where(place == wanted.astype(F32), named, 0.0)
        weight = hit * (jnp.where(is0, gate0, 0.0) + jnp.where(is1, gate1, 0.0))
        top_part = weight.astype(BF)
        hit_ref[k] = hit.astype(BF)
        high_ref[k] = top_part
        low_ref[k] = (weight - top_part.astype(F32)).astype(BF)

    def slot_tables(k):
        placed(k, line // (2 * SLOTS), line % (2 * SLOTS), hits, high, low)
        placed(k, few, jnp.full_like(few, 2 * SLOTS), overs, ohigh, olow)

    slot_tables(7)
    queries_in.wait()
    group = qs.shape[1] // tokens
    for h in range(kv_heads):
        for g in range(group):
            qs[h, tokens * g : tokens * (g + 1), :] = qv[:, HD * (h * group + g) : HD * (h * group + g + 1)]
    stacked = group * tokens
    scale = math.log2(math.e) / math.sqrt(HD)

    def attend(start, count, bias, fresh, h):
        keys = count * 2 * tokens
        k = kv[start : start + count, :, h, 0].reshape(keys, HD)
        v = kv[start : start + count, :, h, 1].reshape(keys, HD)
        scores = lax.dot_general(qs[h], k, (((1,), (1,)), ((), ())), preferred_element_type=F32) * scale + bias
        peak = jnp.max(scores, axis=1, keepdims=True)
        if not fresh:
            peak = jnp.maximum(peak, top[h])
        terms = jnp.exp2(scores - peak).astype(BF)
        both = dot(terms, jnp.concatenate([v, jnp.ones_like(v)], axis=1))
        context, total = both[:, :HD], both[:, HD:]
        if not fresh:
            fade = jnp.exp2(top[h] - peak)
            total = total + mass[h] * fade
            context = context + acc[h] * fade
        top[h], mass[h], acc[h] = peak, total, context

    row = lax.broadcasted_iota(jnp.int32, (stacked, 2 * tokens), 0) % tokens
    col = lax.broadcasted_iota(jnp.int32, (stacked, 2 * tokens), 1)
    diagonal = jnp.where(col <= jnp.where(col < tokens, row, jnp.where(c == 1, 2 * tokens, -1)), 0.0, -1e30)

    def ring_bias(d):
        col = lax.broadcasted_iota(jnp.int32, (1, (2 if d < 4 else 1) * 2 * tokens), 1)
        return jnp.where(jnp.where(col < 2 * tokens, z - d, z + d - NZ) >= 0, 0.0, -1e30)

    def first_step(h, carry):
        swap(7, h).wait_recv()
        attend(7, 1, diagonal, True, h)
        return carry

    lax.fori_loop(0, kv_heads, first_step, 0)
    for d in range(1, 4):
        bias = ring_bias(d - 1) if d > 1 else None

        def ring_step(h, carry, d=d, bias=bias):
            for way in range(2):
                spread(way, d - 1, h).wait_recv()
                if d < 3:
                    spread(way, d, h).start()
                else:
                    pl.when(h // 2 == way)(spread(way, d, h).start)
                swap(slot(way, d), h).start()
            if d > 1:
                for way in range(2):
                    swap(slot(way, d - 1), h).wait_recv()
                attend(slot(0, d - 1), 2, bias, False, h)
            return carry

        lax.fori_loop(0, kv_heads, ring_step, 0)
    bias = ring_bias(3)

    def last_step(h, carry):
        for way in range(2):
            swap(slot(way, 3), h).wait_recv()
        attend(slot(0, 3), 2, bias, False, h)
        return carry

    bias4 = ring_bias(4)
    landed(rz.at[pl.ds(0, 7)], rz_r.at[0])
    for k in range(7):
        slot_tables(k)
    for h in range(2):
        last_step(h, 0)
        for way in range(2):
            spread(way, 3, 2 * way + h).wait_recv()
            swap(6, 2 * way + h).start()
    residual_in.wait()

    own = s == c
    wide = WIDE
    rings = (half - wide) // RING
    ring_half = (tuple(range((rings + 1) // 2)), tuple(range((rings + 1) // 2, rings)))
    hw = half // kv_heads

    def ring_cols(j):
        return pl.ds(wide + RING * j, RING)

    def send(copy, i, same):
        if i == 0 and same:
            pl.when(jnp.logical_not(own))(copy.start)
        else:
            copy.start()

    def settle(ref, sem, axis):
        index = [slice(None)] * len(ref.shape)
        index[axis] = pl.ds(0, ref.shape[axis] - ref.shape[axis] // (16 if ref.shape[axis] > 8 else 8))
        fewer = tuple(pl.ds(0, n) if isinstance(i, slice) else i for i, n in zip(index, ref.shape))

        @pl.when(own)
        def _():
            landed(ref.at[fewer], sem)

        @pl.when(jnp.logical_not(own))
        def _():
            landed(ref, sem)

    def source_rows(ef, cf):
        return pl.ds(pl.multiple_of((ef * 2 + cf) * SLOTS, SLOTS), SLOTS)

    carry_on = {}
    for way in range(2):
        for d in range(4):
            for j in range(2) if d < 3 else (way,):
                at = pl.ds(wide // 2 * j, wide // 2)
                carry_on[way, d, j] = copy_to(
                    hz.at[slot(way, d), :, at], hz.at[slot(way, d + 1), :, at],
                    hz_s.at[way, d // 3], hz_r.at[way, 2 * d + j], ring[way],
                )

    for h in range(kv_heads):
        swap(6, h).wait_recv()
        if h >= 2:
            last_step(h, 0)
        attend(6, 1, bias4, False, h)
        context = acc[h] / mass[h]
        for g in range(group):
            at = slice(HD * (h * group + g), HD * (h * group + g + 1))
            hid[:, at] = (res[:, at].astype(F32) + context[tokens * g : tokens * (g + 1), :]).astype(BF)
        from_col = hw * h
        if from_col < wide:
            to_col = min(wide, from_col + hw)
            hz[7, :, from_col:to_col] = hid[:, from_col:to_col]
            for j in range(2):
                if from_col < wide // 2 * (j + 1) <= to_col:
                    for way in range(2):
                        carry_on[way, 0, j].start()
        if h == 0:
            continue
        a = h - 1
        from_col = max(from_col, wide)
        width = hw * (h + 1) - from_col
        piece = hid[:, from_col : from_col + width]
        part = pl.ds(from_col - wide, width)
        pk[:, :, part] = dot(hits[7], piece).astype(BF).reshape(16, SLOTS, width)
        extra = dot(overs[7], piece)
        for q in range(width // 128):
            pov[a, :, q, :] = extra[:, 128 * q : 128 * (q + 1)]
        land = pl.ds(from_col, width)

        @pl.when(own)
        def _():
            xm[7, source_rows(e, c), land] = pk[e * 2 + s, :, part]
            ovr[a, e] = pov[a, e]

        for i in range(8):
            ed = (e + i) % 8
            for k in (1, 0):
                sd = (s + k) % 2
                send(
                    copy_to(
                        pk.at[ed * 2 + sd, :, part], xm.at[7, source_rows(e, c), land],
                        d_s.at[a], d_r.at[a], (sd, ed, z * 2 + s),
                    ), i, k == 0,
                )
            send(copy_to(pov.at[a, ed], ovr.at[a, e], o_s.at[a], o_r.at[a], (c, ed, z * 2 + s)), i, True)

    groups = ((7, 1), (0, 2), (2, 2), (4, 2), (6, 1))

    def send_wide(w):
        start, count = groups[w]
        for p in range(count):
            tokens_of = hz[start + p]
            pw[w, :, p] = dot(hits[start + p], tokens_of).astype(BF).reshape(16, SLOTS, wide)
            extra = dot(overs[start + p], tokens_of)
            for q in range(wide // 128):
                pvw[w, :, p, q, :] = extra[:, 128 * q : 128 * (q + 1)]
        many = pl.ds(0, count)
        slots = pl.ds(start, count)
        at = pl.ds(0, wide)

        @pl.when(own)
        def _():
            xm[slots, source_rows(e, c), at] = pw[w, e * 2 + s, many]
            ovw[w, e, many] = pvw[w, e, many]

        for i in range(8):
            ed = (e + i) % 8
            for k in (1, 0):
                sd = (s + k) % 2
                send(
                    copy_to(
                        pw.at[w, ed * 2 + sd, many], xm.at[slots, source_rows(e, c), at],
                        dw_s.at[w], dw_r.at[w], (sd, ed, z * 2 + s),
                    ), i, k == 0,
                )
            send(
                copy_to(pvw.at[w, ed, many], ovw.at[w, e, many], ow_s.at[w], ow_r.at[w], (c, ed, z * 2 + s)),
                i, True,
            )

    def receive_wide(w):
        start, count = groups[w]
        many = pl.ds(0, count)
        slots = pl.ds(start, count)
        at = pl.ds(0, wide)
        settle(xm.at[slots, pl.ds(0, MAIN), at], dw_r.at[w], 1)
        settle(ovw.at[w, :, many], ow_r.at[w], 0)
        for p in range(count):
            for q in range(wide // 128):
                xm[start + p, MAIN:, 128 * q : 128 * (q + 1)] = ovw[w, :, p, q, :].astype(BF)
            share[start + p, 0].start()

    def carry(d):
        for j in range(2):
            for way in range(2) if d < 4 else (j,):
                carry_on[way, d - 1, j].wait_recv()
                if (way, d, j) in carry_on:
                    carry_on[way, d, j].start()

    def cols(j):
        return pl.ds(cw * j, cw)

    half_of = ((0, 1), (2, 3))
    gather, share = {}, {}
    split = wide + 3 * RING
    parts = ((0, wide), (wide, split), (split, half))
    for way in range(2):
        for d in range(4):
            for j in range(rings) if d < 3 else ring_half[way]:
                n = d * rings + j
                gather[way, d, j] = copy_to(
                    xm.at[slot(way, d), :, ring_cols(j)], xm.at[slot(way, d + 1), :, ring_cols(j)],
                    ag_s.at[way, d // 3], ag_r.at[way, n], ring[way],
                )
    for k in range(8):
        for n, (begin, end) in enumerate(parts):
            at = pl.ds(begin, end - begin)
            share[k, n] = copy_to(xm.at[k, :, at], xp.at[k, :, at], xs.at[0], xrs.at[k, n], partner)

    def trade(g, j):
        at = pl.ds(pl.multiple_of(j * cw, cw), cw)
        pair = pl.ds(2 * g - 2, 2)
        return copy_to(yps.at[pair, :, at], ypr.at[pair, :, at], yss.at[0], yrs.at[g - 1, j], partner)

    def hidden_units(g, first, last):
        def piece(k, carry):
            at = pl.ds(pl.multiple_of(k * 256, 256), 256)
            left = xm[2 * g - 2 : 2 * g].reshape(2 * ROWS, half)
            right = xp[2 * g - 2 : 2 * g].reshape(2 * ROWS, half)
            gate = dot(left, wg[0, :, at]) + dot(right, wg[1, :, at])
            lift = dot(left, wu[0, :, at]) + dot(right, wu[1, :, at])
            inner[pl.ds((2 * g - 2) * ROWS, 2 * ROWS), at] = (gate / (1.0 + jnp.exp(-gate)) * lift).astype(BF)
            return carry

        lax.fori_loop(first, last, piece, 0)

    def units_part(g, n, fresh, done):
        begin, end = parts[n]
        at_k = pl.ds(begin, end - begin)

        def piece(k, carry):
            at = pl.ds(pl.multiple_of(k * 256, 256), 256)
            left = xm[2 * g - 2 : 2 * g, :, at_k].reshape(2 * ROWS, end - begin)
            right = xp[2 * g - 2 : 2 * g, :, at_k].reshape(2 * ROWS, end - begin)
            gate = dot(left, wg[0, at_k, at]) + dot(right, wg[1, at_k, at])
            lift = dot(left, wu[0, at_k, at]) + dot(right, wu[1, at_k, at])
            if not fresh:
                gate, lift = gate + partial[0, :, at], lift + partial[1, :, at]
            if done:
                inner[pl.ds((2 * g - 2) * ROWS, 2 * ROWS), at] = (gate / (1.0 + jnp.exp(-gate)) * lift).astype(BF)
            else:
                partial[0, :, at], partial[1, :, at] = gate, lift
            return carry

        lax.fori_loop(0, 2, piece, 0)

    def down_out(g):
        rows = inner[pl.ds((2 * g - 2) * ROWS, 2 * ROWS), :]

        def theirs(j, carry):
            at = pl.ds(pl.multiple_of(j * cw, cw), cw)
            yps[pl.ds(2 * g - 2, 2), :, at] = dot(rows, wd[1, :, at]).astype(BF).reshape(2, ROWS, cw)
            trade(g, j).start()
            return carry

        lax.fori_loop(0, CHUNKS, theirs, 0)

    def down_own(g):
        rows = inner[pl.ds((2 * g - 2) * ROWS, 2 * ROWS), :]

        def mine(j, carry):
            trade(g, j).wait_recv()
            at = pl.ds(pl.multiple_of(j * cw, cw), cw)
            both = dot(rows, wd[0, :, at]).reshape(2, ROWS, cw) + ypr[pl.ds(2 * g - 2, 2), :, at].astype(F32)
            ys[pl.ds(2 * g - 2, 2), :, at] = both.astype(BF)
            return carry

        lax.fori_loop(0, CHUNKS, mine, 0)

    reduce, link = {}, {}
    for way in range(2):
        for d in range(1, 5):
            target = slot(1 - way, d)
            for j in range(rings) if d < 4 else ring_half[way]:
                n = (d - 1) * rings + j
                reduce[way, d, j] = copy_to(
                    ys.at[target, :, ring_cols(j)], rr.at[way, d - 1, :, pl.ds(RING * j, RING)],
                    rs_s.at[way, d // 4], rs_r.at[way, n], ring[way],
                )
            for j in range(2) if d < 4 else (way,):
                at = pl.ds(wide // 2 * j, wide // 2)
                link[way, d, j] = copy_to(
                    cz.at[target, :, at], rc.at[way, d - 1, :, at],
                    cr_s.at[way, d // 4], cr_r.at[way, 2 * (d - 1) + j], ring[way],
                )

    def pass_on(way, d, j, add):
        if add:
            reduce[way, d + 1, j].wait_recv()
            k = slot(1 - way, d)
            total = ys[k, :, ring_cols(j)].astype(F32) + rr[way, d, :, pl.ds(RING * j, RING)].astype(F32)
            ys[k, :, ring_cols(j)] = total.astype(BF)
        reduce[way, d, j].start()

    def both_ways(d, lists, add):
        for n in range(max(len(lists[0]), len(lists[1]))):
            for way in range(2):
                if n < len(lists[way]):
                    pass_on(way, d, lists[way][n], add)

    def chain(d):
        for j in range(2):
            at = pl.ds(wide // 2 * j, wide // 2)
            for way in range(2):
                if (way, d, j) in link:
                    if (way, d + 1, j) in link:
                        link[way, d + 1, j].wait_recv()
                        k = slot(1 - way, d)
                        cz[k, :, at] = (cz[k, :, at].astype(F32) + rc[way, d, :, at].astype(F32)).astype(BF)
                    link[way, d, j].start()

    def weigh(k, rows, extra):
        return (
            dot_rows(high[k], rows) + dot_rows(low[k], rows) + dot_rows(ohigh[k], extra) + dot_rows(olow[k], extra)
        )

    def send_back(w):
        start, count = groups[w]
        many, slots, at = pl.ds(0, count), pl.ds(start, count), pl.ds(0, wide)
        for p in range(count):
            tail = ys[start + p, MAIN:, at].astype(F32)
            for q in range(wide // 128):
                pvb[w, :, p, q, :] = tail[:, 128 * q : 128 * (q + 1)]

        @pl.when(own)
        def _():
            rb[w, e * 2 + s, many] = ys[slots, source_rows(e, c), at]
            ovb[w, e, many] = pvb[w, e, many]

        for i in range(8):
            ed = (e + i) % 8
            for k in (1, 0):
                cd = (c + k) % 2
                send(
                    copy_to(
                        ys.at[slots, source_rows(ed, cd), at], rb.at[w, e * 2 + s, many],
                        bw_s.at[w], bw_r.at[w], (c, ed, z * 2 + cd),
                    ), i, k == 0,
                )
            send(
                copy_to(pvb.at[w, ed, many], ovb.at[w, e, many], vw_s.at[w], vw_r.at[w], (c, ed, z * 2 + s)),
                i, True,
            )

    def receive_back(w):
        start, count = groups[w]
        many, slots, at = pl.ds(0, count), pl.ds(start, count), pl.ds(0, wide)
        settle(rb.at[w, :, many], bw_r.at[w], 0)
        settle(ovb.at[w, :, many], vw_r.at[w], 0)
        totals = []
        for p in range(count):
            extra = jnp.concatenate([ovb[w, :, p, q, :] for q in range(wide // 128)], axis=1).astype(BF)
            totals.append(weigh(start + p, rb[w, :, p].reshape(MAIN, wide), extra))
            if w > 0:
                cz[start + p] = totals[p].astype(BF)
        return totals[0]

    send_wide(0)
    carry(1)
    send_wide(1)
    for a in range(3):
        from_col = max(wide, hw * (a + 1))
        width = hw * (a + 2) - from_col
        land = pl.ds(from_col, width)
        part = pl.ds(from_col - wide, width)
        settle(xm.at[7, pl.ds(0, MAIN), land], d_r.at[a], 0)
        settle(ovr.at[a], o_r.at[a], 0)
        for q in range(width // 128):
            at = from_col + 128 * q
            xm[7, MAIN:, at : at + 128] = ovr[a, :, q, :].astype(BF)
        for j in range((from_col - wide) // RING, (from_col - wide + width) // RING):
            for way in range(2):
                gather[way, 0, j].start()
        if a == 1:
            carry(2)
    share[7, 1].start()
    share[7, 2].start()
    send_wide(2)
    carry(3)
    send_wide(3)
    for load in loads:
        load.wait()

    receive_wide(0)

    def shared(k):
        for n in range(3):
            share[k, n].wait_recv()

    for d in range(1, 4):
        if d > 1:
            receive_wide(d - 1)
            for way in range(2):
                shared(slot(way, d - 1))
        for j in range(rings):
            for way in range(2):
                gather[way, d - 1, j].wait_recv()
                if (way, d, j) in gather:
                    gather[way, d, j].start()
                if j in (2, rings - 1):
                    share[slot(way, d), 1 + j // 3].start()
            if d == 1 and j == 1:
                carry(4)
                send_wide(4)
            if d > 1 and j in (1, 3):
                hidden_units(d - 1, j // 2, j // 2 + 1)
            if d == 3 and j == 2:
                receive_wide(3)
            if d == 3 and j == 3:
                for way in range(2):
                    share[slot(way, 3), 1].wait_recv()
                units_part(3, 1, True, False)
    for way in range(2):
        share[slot(way, 3), 2].wait_recv()
    units_part(3, 2, False, False)
    for way in range(2):
        share[slot(way, 3), 0].wait_recv()
    units_part(3, 0, False, True)
    down_out(3)
    receive_wide(4)
    for way in range(2):
        for j in ring_half[way]:
            gather[way, 3, j].wait_recv()
    share[6, 1].start()
    share[6, 2].start()
    down_own(3)

    swapped = (ring_half[1], ring_half[0])
    orders = tuple(b + a for a, b in zip(ring_half, swapped))
    lasts = (orders[0], (0, 3, 4, 1, 2))
    both_ways(3, swapped, False)
    send_back(3)
    down_out(2)
    shared(6)
    shared(7)
    hidden_units(4, 0, 2)
    down_out(4)
    down_own(2)
    both_ways(2, swapped, True)
    down_own(4)
    both_ways(4, ring_half, False)
    send_back(4)
    send_back(2)
    down_out(1)
    receive_back(3)
    both_ways(3, ring_half, True)
    receive_back(4)
    chain(4)
    down_own(1)
    send_back(1)
    send_back(0)
    both_ways(2, ring_half, True)
    chain(3)
    receive_back(2)
    both_ways(1, tuple(o[:2] for o in lasts), True)
    both_ways(1, tuple(o[2:4] for o in lasts), True)
    chain(2)
    receive_back(1)
    both_ways(1, tuple(o[4:] for o in lasts), True)
    chain(1)

    pieces = ((3, 2), (0, 2), (2, 1))
    for a, (j, count) in enumerate(pieces):
        width = count * RING
        for n in range(j, j + count):
            for way in range(2):
                reduce[way, 1, n].wait_recv()
        land, part = pl.ds(wide + RING * j, width), pl.ds(RING * j, width)
        total = (
            ys[7, :, land].astype(F32) + rr[0, 0, :, part].astype(F32) + rr[1, 0, :, part].astype(F32)
        ).astype(BF)
        ys[7, :, land] = total
        tail = total[MAIN:].astype(F32)
        for q in range(width // 128):
            fov[a, :, q, :] = tail[:, 128 * q : 128 * (q + 1)]

        @pl.when(own)
        def _():
            ret[e * 2 + s, :, part] = ys[7, source_rows(e, c), land]
            retov[a, e] = fov[a, e]

        for i in range(8):
            ed = (e + i) % 8
            for k in (1, 0):
                cd = (c + k) % 2
                send(
                    copy_to(
                        ys.at[7, source_rows(ed, cd), land], ret.at[e * 2 + s, :, part],
                        b_s.at[a], b_r.at[a], (c, ed, z * 2 + cd),
                    ), i, k == 0,
                )
            send(copy_to(fov.at[a, ed], retov.at[a, e], bo_s.at[a], bo_r.at[a], (c, ed, z * 2 + s)), i, True)

    total = receive_back(0)
    for way in range(2):
        for j in range(2):
            link[way, 1, j].wait_recv()
        total = total + rc[way, 0].astype(F32)
    out[0, :, 0:wide] = (hid[:, 0:wide].astype(F32) + total).astype(BF)

    for a, (j, count) in enumerate(pieces):
        width = count * RING
        land, part = pl.ds(wide + RING * j, width), pl.ds(RING * j, width)
        settle(ret.at[:, :, part], b_r.at[a], 0)
        settle(retov.at[a], bo_r.at[a], 0)
        extra = jnp.concatenate([retov[a, :, q, :] for q in range(width // 128)], axis=1).astype(BF)
        total = weigh(7, ret[:, :, part].reshape(MAIN, width), extra)
        out[0, :, land] = (hid[:, land].astype(F32) + total).astype(BF)

    for a in range(3):
        from_col = max(wide, hw * (a + 1))
        part = pl.ds(from_col - wide, hw * (a + 2) - from_col)
        settle(pk.at[:, :, part], d_s.at[a], 0)
        settle(pov.at[a], o_s.at[a], 0)
        settle(ret.at[:, :, pl.ds(RING * pieces[a][0], RING * pieces[a][1])], b_s.at[a], 0)
        settle(fov.at[a], bo_s.at[a], 0)
    for w, (start, count) in enumerate(groups):
        many = pl.ds(0, count)
        settle(pw.at[w, :, many], dw_s.at[w], 0)
        settle(pvw.at[w, :, many], ow_s.at[w], 0)
        settle(rb.at[w, :, many], bw_s.at[w], 0)
        settle(pvb.at[w, :, many], vw_s.at[w], 0)
    some = pl.ds(0, 3)
    rest = pl.ds(0, wide // 2)
    for way in range(2):
        landed(kv.at[some, 0], kg_s.at[way, 0])
        landed(kv.at[0, 0, pl.ds(0, 2)], kg_s.at[way, 1])
        landed(hz.at[some], hz_s.at[way, 0])
        landed(hz.at[0, :, rest], hz_s.at[way, 1])
        landed(xm.at[some, :, pl.ds(wide, half - wide)], ag_s.at[way, 0])
        landed(xm.at[0, :, pl.ds(wide, RING * len(ring_half[way]))], ag_s.at[way, 1])
        landed(ys.at[some, :, pl.ds(wide, half - wide)], rs_s.at[way, 0])
        landed(ys.at[0, :, pl.ds(wide, RING * len(ring_half[way]))], rs_s.at[way, 1])
        landed(cz.at[some], cr_s.at[way, 0])
        landed(cz.at[0, :, rest], cr_s.at[way, 1])
    landed(kv.at[:, 0], kx_s.at[0])
    landed(rz.at[pl.ds(0, 7)], rz_s.at[0])
    landed(xm, xs.at[0])
    landed(yps, yss.at[0])


def on_device(query, keys, values, residual, routes, gates, w_gate, w_up, w_down):
    _, tokens, half = query.shape
    units = w_gate.shape[2]
    kv_heads = keys.shape[2] // HD
    stacked = half // HD // kv_heads * tokens
    vmem = pl.BlockSpec(memory_space=pltpu.VMEM)
    hbm = pl.BlockSpec(memory_space=pl.ANY)
    dma = pltpu.SemaphoreType.DMA
    return pl.pallas_call(
        layer_kernel,
        out_shape=jax.ShapeDtypeStruct(query.shape, BF),
        in_specs=[hbm] * 4 + [vmem] * 2 + [hbm] * 3,
        out_specs=vmem,
        scratch_shapes=[
            pltpu.VMEM((tokens, half), BF),
            pltpu.VMEM((tokens, half), BF),
            pltpu.VMEM((8, 2, kv_heads, 2, tokens, HD), BF),
            pltpu.VMEM((kv_heads, stacked, HD), BF),
            pltpu.VMEM((kv_heads, stacked, 1), F32),
            pltpu.VMEM((kv_heads, stacked, HD), F32),
            pltpu.VMEM((kv_heads, stacked, HD), F32),
            pltpu.VMEM((tokens, half), BF),
            pltpu.VMEM((8, 8, 128), F32),
            pltpu.VMEM((8, MAIN, tokens), BF),
            pltpu.VMEM((8, EXPERTS, tokens), BF),
            pltpu.VMEM((8, MAIN, tokens), BF),
            pltpu.VMEM((8, MAIN, tokens), BF),
            pltpu.VMEM((8, EXPERTS, tokens), BF),
            pltpu.VMEM((8, EXPERTS, tokens), BF),
            pltpu.VMEM((8, tokens, WIDE), BF),
            pltpu.VMEM((2, half, units), BF),
            pltpu.VMEM((2, half, units), BF),
            pltpu.VMEM((2, units, half), BF),
            pltpu.VMEM((16, SLOTS, half - WIDE), BF),
            pltpu.VMEM((3, 8, 8, 128), F32),
            pltpu.VMEM((3, 8, 8, 128), F32),
            pltpu.VMEM((5, 16, 2, SLOTS, WIDE), BF),
            pltpu.VMEM((5, 8, 2, 8, 128), F32),
            pltpu.VMEM((5, 8, 2, 8, 128), F32),
            pltpu.VMEM((8, ROWS, half), BF),
            pltpu.VMEM((8, ROWS, half), BF),
            pltpu.VMEM((2, 2 * ROWS, units), F32),
            pltpu.VMEM((8 * ROWS, units), BF),
            pltpu.VMEM((8, ROWS, half), BF),
            pltpu.VMEM((8, ROWS, half), BF),
            pltpu.VMEM((8, ROWS, half), BF),
            pltpu.VMEM((2, 4, ROWS, half - WIDE), BF),
            pltpu.VMEM((3, 8, 8, 128), F32),
            pltpu.VMEM((16, SLOTS, half - WIDE), BF),
            pltpu.VMEM((3, 8, 8, 128), F32),
            pltpu.VMEM((5, 16, 2, SLOTS, WIDE), BF),
            pltpu.VMEM((5, 8, 2, 8, 128), F32),
            pltpu.VMEM((5, 8, 2, 8, 128), F32),
            pltpu.VMEM((8, tokens, WIDE), BF),
            pltpu.VMEM((2, 4, tokens, WIDE), BF),
            dma((3,)), dma((1,)), dma((1,)), dma((2, 2)), dma((2, 16)), dma((1,)), dma((8, 4)),
            dma((2, 2)), dma((2, 8)), dma((5,)), dma((5,)), dma((5,)), dma((5,)),
            dma((6,)), dma((3,)), dma((3,)), dma((3,)), dma((3,)),
            dma((2, 2)), dma((2, 20)), dma((1,)), dma((8, 3)), dma((1,)), dma((4, 4)),
            dma((2, 2)), dma((2, 20)), dma((3,)), dma((3,)), dma((3,)), dma((3,)),
            dma((5,)), dma((5,)), dma((5,)), dma((5,)), dma((2, 2)), dma((2, 8)),
        ],
        compiler_params=pltpu.CompilerParams(
            collective_id=1, has_side_effects=True, vmem_limit_bytes=60 * 1024 * 1024
        ),
        name="layer",
    )(query, keys, values, residual, routes[0].T, gates[0].T, w_gate, w_up, w_down)


def solution(mesh):
    return jax.shard_map(
        on_device,
        mesh=mesh,
        in_specs=(
            P("expert", "tensor", "section"),
            P("expert", "tensor", "section"),
            P("expert", "tensor", "section"),
            P("expert", "tensor", "section"),
            P("expert", "tensor", None),
            P("expert", "tensor", None),
            P("expert", None, "tensor"),
            P("expert", None, "tensor"),
            P("expert", "tensor", None),
        ),
        out_specs=P("expert", "tensor", "section"),
        check_vma=False,
    )
```
